32 devices in a mesh: inst: 2 (over x), qy: 4 (over z), qx: 4 (over y, core).
Axes of the slice: x: 2, y: 2, z: 4, core: 2. Of those that a mesh axis runs over, the one named last changes fastest.
Arguments:
- cost: float32 [2097152], P(('inst', 'qy', 'qx')), parts along dimension 0
- gamma: float32 [4, 5], P('inst'), parts along dimension 0
- beta: float32 [4, 5], P('inst'), parts along dimension 0
Outputs:
- output 1: float32 [4], P('inst'), parts along dimension 0
- output 2: float32 [4, 10], P('inst'), parts along dimension 0
There are 2 independent parts. The reference program is written for one: setup_inputs(seed, part) draws one part's arguments, and reference() takes and returns one part's arrays. A program takes and returns all parts, laid end to end along the dimension named above; each array names one.
All inputs are finite; a program needn't handle non-finite values.
Results may differ from the reference program's by a relative error of at most 0.001.
Values sent between devices are 32-bit elements.
A program may use at most 1 GiB of HBM per device.

```python
import functools
import jax
import jax.numpy as jnp
from jax import lax

QUBITS = 20
LAYERS = 5
DEGREE = 3


def bit_table(count):
    index = jnp.arange(2 ** count, dtype=jnp.int32)[:, None]
    return ((index >> jnp.arange(count, dtype=jnp.int32)[None, :]) & 1).astype(jnp.float32)


def cut_values(adjacency):
    low_count = QUBITS // 2
    high_count = QUBITS - low_count
    low_bits = bit_table(low_count)
    high_bits = bit_table(high_count)
    degrees = jnp.sum(adjacency, axis=1)
    highest = lax.Precision.HIGHEST
    low_term = jnp.dot(low_bits, degrees[:low_count], precision=highest) - jnp.sum(jnp.dot(low_bits, adjacency[:low_count, :low_count], precision=highest) * low_bits, axis=1)
    high_term = jnp.dot(high_bits, degrees[low_count:], precision=highest) - jnp.sum(jnp.dot(high_bits, adjacency[low_count:, low_count:], precision=highest) * high_bits, axis=1)
    cross_term = jnp.dot(jnp.dot(high_bits, adjacency[low_count:, :low_count], precision=highest), low_bits.T, precision=highest)
    cut = high_term[:, None] + low_term[None, :] - 2.0 * cross_term
    total_weight = 0.5 * jnp.sum(adjacency)
    spread = jnp.sqrt(0.5 * jnp.sum(adjacency * adjacency))
    return ((cut - 0.5 * total_weight) * (2.0 / spread)).reshape(-1)


def draw_cost(cost_key):
    key_dst, key_weight = jax.random.split(cost_key)
    num_edges = QUBITS * DEGREE // 2
    edge_src = jnp.arange(num_edges, dtype=jnp.int32) % QUBITS
    edge_dst = (edge_src + jax.random.randint(key_dst, (num_edges,), 1, QUBITS)) % QUBITS
    weight_tilt = 0.5 + (edge_src + edge_dst).astype(jnp.float32) / QUBITS
    edge_weight = jax.random.uniform(key_weight, (num_edges,), jnp.float32, 0.5, 1.5) * weight_tilt
    adjacency = jnp.zeros((QUBITS, QUBITS), jnp.float32).at[edge_src, edge_dst].add(edge_weight)
    return cut_values(adjacency + adjacency.T)


def setup_inputs(seed: int = 0, part: int = 0) -> dict:
    base_key = jax.random.fold_in(jax.random.key(seed), part)
    key_cost, key_gamma, key_beta = jax.random.split(base_key, 3)
    cost = draw_cost(key_cost)
    gamma = jax.random.uniform(key_gamma, (2, LAYERS), jnp.float32, 0.2, 1.0)
    beta = jax.random.uniform(key_beta, (2, LAYERS), jnp.float32, 0.6, 2.4)
    return {"cost": cost, "gamma": gamma, "beta": beta}


def flip_bit(amplitudes, qubit):
    return jnp.flip(amplitudes.reshape(-1, 2, 2 ** qubit), axis=1).reshape(-1)


def one_set(cost, angles):
    gamma_row, beta_row = angles
    start = jnp.full(cost.shape, 2.0 ** (-0.5 * QUBITS), jnp.float32)

    def forward_layer(state, layer_angles):
        psi_re, psi_im = state
        gamma_l, beta_l = layer_angles
        phase = gamma_l * cost
        cos_p = jnp.cos(phase)
        sin_p = jnp.sin(phase)
        psi_re, psi_im = psi_re * cos_p + psi_im * sin_p, psi_im * cos_p - psi_re * sin_p
        cos_b = jnp.cos(0.5 * beta_l)
        sin_b = jnp.sin(0.5 * beta_l)
        for qubit in range(QUBITS):
            flip_re = flip_bit(psi_re, qubit)
            flip_im = flip_bit(psi_im, qubit)
            psi_re, psi_im = cos_b * psi_re + sin_b * flip_im, cos_b * psi_im - sin_b * flip_re
        return (psi_re, psi_im), None

    final_state = lax.scan(forward_layer, (start, jnp.zeros_like(start)), (gamma_row, beta_row))[0]
    psi_re, psi_im = final_state
    energy = jnp.sum(cost * (psi_re * psi_re + psi_im * psi_im))

    def backward_layer(state, layer_angles):
        psi_re, psi_im, lam_re, lam_im = state
        gamma_l, beta_l = layer_angles
        cos_b = jnp.cos(0.5 * beta_l)
        sin_b = jnp.sin(0.5 * beta_l)
        beta_grad = jnp.zeros((), jnp.float32)
        for qubit in range(QUBITS):
            flip_psi_re = flip_bit(psi_re, qubit)
            flip_psi_im = flip_bit(psi_im, qubit)
            flip_lam_re = flip_bit(lam_re, qubit)
            flip_lam_im = flip_bit(lam_im, qubit)
            beta_grad = beta_grad + jnp.sum(lam_re * flip_psi_im - lam_im * flip_psi_re)
            psi_re, psi_im = cos_b * psi_re - sin_b * flip_psi_im, cos_b * psi_im + sin_b * flip_psi_re
            lam_re, lam_im = cos_b * lam_re - sin_b * flip_lam_im, cos_b * lam_im + sin_b * flip_lam_re
        gamma_grad = 2.0 * jnp.sum(cost * (lam_re * psi_im - lam_im * psi_re))
        phase = gamma_l * cost
        cos_p = jnp.cos(phase)
        sin_p = jnp.sin(phase)
        psi_re, psi_im = psi_re * cos_p - psi_im * sin_p, psi_im * cos_p + psi_re * sin_p
        lam_re, lam_im = lam_re * cos_p - lam_im * sin_p, lam_im * cos_p + lam_re * sin_p
        return (psi_re, psi_im, lam_re, lam_im), (gamma_grad, beta_grad)

    layer_grads = lax.scan(backward_layer, (psi_re, psi_im, cost * psi_re, cost * psi_im), (gamma_row, beta_row), reverse=True)[1]
    return energy, jnp.concatenate([layer_grads[0], layer_grads[1]])


def reference(cost, gamma, beta):
    energy, grad = lax.map(functools.partial(one_set, cost), (gamma, beta))
    return (energy, grad)
```

```python
import functools
import jax
import jax.numpy as jnp
from jax import lax
from jax.experimental import pallas as pl
from jax.experimental.pallas import tpu as pltpu
from jax.sharding import PartitionSpec as P

F32 = jnp.float32
BF16 = jnp.bfloat16
LAYERS = 5
LOCAL_QUBITS = 19
CHUNK = 64
NUM_CHUNKS = 256 // CHUNK
NUM_ACC = 16
MESH = pl.DeviceIdType.MESH
HOMES = ((1, 0), (2, 2))


def sincos(x):
    magic = 12582912.0
    k = (x * 0.6366197723675814 + magic) - magic
    r = ((x - k * 1.5703125) - k * 4.837512969970703125e-4) - k * 7.54978995489188216e-8
    z = r * r
    sin_r = ((-1.9515295891e-4 * z + 8.3321608736e-3) * z - 1.6666654611e-1) * (z * r) + r
    cos_r = ((2.443315711809948e-5 * z - 1.388731625493765e-3) * z + 4.166664568298827e-2) * (z * z) - (0.5 * z - 1.0)
    quad = k.astype(jnp.int32)
    odd = (quad & 1) == 1
    sin_x = jnp.where(odd, cos_r, sin_r)
    cos_x = jnp.where(odd, sin_r, cos_r)
    sin_x = jnp.where((quad & 2) == 2, -sin_x, sin_x)
    cos_x = jnp.where(((quad + 1) & 2) == 2, -cos_x, cos_x)
    return sin_x, cos_x


def split3(x):
    a = x.astype(BF16)
    r = x - a.astype(F32)
    b = r.astype(BF16)
    c = (r - b.astype(F32)).astype(BF16)
    return a, b, c


def butterfly8(v):
    for step in (4, 2, 1):
        out = list(v)
        for i in range(8):
            if not i & step:
                out[i] = v[i] + v[i + step]
                out[i + step] = v[i] - v[i + step]
        v = out
    return v


def popcount_tile(shape):
    sub = lax.broadcasted_iota(jnp.int32, shape, 0)
    lane = lax.broadcasted_iota(jnp.int32, shape, 1)
    total = jnp.zeros(shape, jnp.int32)
    for b in range(3):
        total = total + ((sub >> b) & 1)
    for b in range(7):
        total = total + ((lane >> b) & 1)
    return total.astype(F32)


def fold(x):
    return jnp.sum(x.reshape(-1, 8, 128), axis=0)


def dot3(lhs, rhs):
    return sum(jnp.dot(a, b, preferred_element_type=F32) for a, b in zip(lhs, rhs))


def cols_of(ct):
    return pl.ds(ct * 128, 128)


def rotate(values, cos_b, sin_b):
    kr, ki, orr, oi = values
    return (cos_b * kr + sin_b * oi, cos_b * ki - sin_b * orr, cos_b * orr + sin_b * ki, cos_b * oi - sin_b * kr)


def groups(i):
    for g in range(CHUNK // 16):
        for ct in range(2):
            start = pl.multiple_of(i * CHUNK + g * 16, 16)
            cost_start = pl.multiple_of(ct * 256 + i * CHUNK + g * 16, 16)
            yield pl.ds(g * 16, 16), pl.ds(start, 16), cols_of(ct), pl.ds(cost_start, 16)


def loop(count, body):
    def step(n, carry):
        body(n)
        return carry
    lax.fori_loop(0, count, step, 0)


def kernel(cost, gamma, beta, had, out, stash, keep, other, cc, tab, saved, hat, diag, rot, acc,
           parts, wide, big, mine, res, c_send, c_recv, f_send, f_recv, x_send, x_recv, h_out, h_in, r_send, r_recv, credit):
    inst = lax.axis_index('inst')
    qy = lax.axis_index('qy')
    qx = lax.axis_index('qx')
    core = lax.rem(qx, 2)
    my_set = qx // 2
    active = qy == my_set + 1
    partner = (inst, qy, qx + 1 - 2 * core)
    kind = lax.rem(qy // 2 + qy, 2)

    def cost_copy(s):
        home_y, home_x = HOMES[s]
        return pltpu.make_async_remote_copy(
            src_ref=cost, dst_ref=cc.at[kind, qx], send_sem=c_send.at[s], recv_sem=c_recv.at[kind, qx],
            device_id=(inst, home_y, home_x + qy // 2), device_id_type=MESH)

    def is_self(s):
        home_y, home_x = HOMES[s]
        return (qy == home_y) & (qx == home_x + qy // 2)

    for s in range(2):
        @pl.when(is_self(s))
        def _():
            pltpu.make_async_copy(cost, cc.at[kind, qx], c_recv.at[kind, qx]).start()

        @pl.when(jnp.logical_not(is_self(s)))
        def _():
            cost_copy(s).start()

    def cost_arrived(which, j):
        pltpu.make_async_copy(cost, cc.at[which, j], c_recv.at[which, j]).wait()

    def forward_copy(j):
        return pltpu.make_async_remote_copy(
            src_ref=cc.at[1, j], dst_ref=cc.at[2, j], send_sem=f_send.at[j], recv_sem=f_recv.at[j],
            device_id=partner, device_id_type=MESH)

    def exchange(parity, i):
        rows = pl.ds(pl.multiple_of(i * CHUNK, CHUNK), CHUNK)
        return pltpu.make_async_remote_copy(
            src_ref=other.at[1 - parity, :, :, rows, :], dst_ref=other.at[parity, :, :, rows, :],
            send_sem=x_send.at[parity, i], recv_sem=x_recv.at[parity, i],
            device_id=partner, device_id_type=MESH)

    def release(i):
        pl.semaphore_signal(credit.at[i], inc=1, device_id=partner, device_id_type=MESH)

    def send(parity, i, first=None):
        if first is None:
            pl.semaphore_wait(credit.at[i], 1)
        else:
            @pl.when(jnp.logical_not(first))
            def _():
                pl.semaphore_wait(credit.at[i], 1)
        exchange(parity, i).start()

    def stash_out(n):
        return pltpu.make_async_copy(hat.at[lax.rem(n, 2)], stash.at[n], h_out.at[lax.rem(n, 2)])

    def stash_in(n):
        return pltpu.make_async_copy(stash.at[n], hat.at[lax.rem(n, 2)], h_in.at[lax.rem(n, 2)])

    def put_parts(t, rows, cols, x):
        for p, piece in enumerate(split3(x)):
            parts[p, t, rows, cols] = piece

    def right_multiply(write):
        h = had[...]
        for t in range(0, 16, 4):
            lhs = [parts[p, t:t + 4].reshape(4 * CHUNK, 256) for p in range(3)]
            write(t, dot3(lhs, (h, h, h)).reshape(4, CHUNK, 256))

    def state_write(par, i):
        rows = pl.ds(pl.multiple_of(i * CHUNK, CHUNK), CHUNK)

        def write(t, value):
            comp, half = t // 8, (t // 4) % 2
            if half == 0:
                keep[comp, :, rows, :] = value
            else:
                other[par, comp, :, rows, :] = value
        return write

    def big_write(t, value):
        big[t:t + 4] = value

    def load_state(par, rows, cols, j):
        return (keep[0, j, rows, cols], keep[1, j, rows, cols],
                other[par, 0, j, rows, cols], other[par, 1, j, rows, cols])

    def store_state(par, rows, cols, j, values):
        keep[0, j, rows, cols] = values[0]
        keep[1, j, rows, cols] = values[1]
        other[par, 0, j, rows, cols] = values[2]
        other[par, 1, j, rows, cols] = values[3]

    def spread(re, im, local_rows, cols):
        for comp, v in enumerate((butterfly8(re), butterfly8(im))):
            for t in range(8):
                put_parts(comp * 8 + t, local_rows, cols, v[t])

    def gather_big(local_rows, cols):
        re = butterfly8([big[t, local_rows, cols] for t in range(8)])
        im = butterfly8([big[8 + t, local_rows, cols] for t in range(8)])
        return re, im

    def inverse_chunk(par, i):
        for g in range(CHUNK // 16):
            rows = pl.ds(pl.multiple_of(i * CHUNK + g * 16, 16), 16)
            for ct in range(2):
                for j in range(4):
                    v = load_state(par, rows, cols_of(ct), j)
                    for t, x in zip((j, 8 + j, 4 + j, 12 + j), v):
                        put_parts(t, pl.ds(g * 16, 16), cols_of(ct), x)
        right_multiply(big_write)

    def middle(layer, par, forward):
        h = had[...]
        slot = lax.rem(layer, 2)

        def block(j, total, half):
            n = half * 4 + j
            bits = half + j // 2 + lax.rem(j, 2)
            for comp in range(2):
                src = keep[comp, j] if half == 0 else other[par, comp, j]
                wide[comp] = dot3((h, h, h), split3(src))
            for g in range(16):
                rows = pl.ds(g * 16, 16)
                for ct in range(2):
                    cols = cols_of(ct)
                    q0 = bin(2 * g).count('1') + ct
                    q1 = bin(2 * g + 1).count('1') + ct

                    def pick(m):
                        return jnp.concatenate([diag[layer, m, bits + q0], diag[layer, m, bits + q1]], axis=0)
                    re, im = wide[0, rows, cols], wide[1, rows, cols]
                    dc, ds = pick(0), pick(1)
                    if forward:
                        re, im = re * dc + im * ds, im * dc - re * ds
                        hat[slot, 0, n, rows, cols] = re
                        hat[slot, 1, n, rows, cols] = im
                    else:
                        term = re * hat[slot, 1, n, rows, cols] - im * hat[slot, 0, n, rows, cols]
                        total = total + fold(term * pick(2))
                        re, im = re * dc - im * ds, im * dc + re * ds
                    wide[0, rows, cols] = re
                    wide[1, rows, cols] = im
            for comp in range(2):
                value = dot3((h, h, h), split3(wide[comp]))
                if half == 0:
                    keep[comp, j] = value
                else:
                    other[par, comp, j] = value
            return total

        def body(j, total):
            return block(j, block(j, total, 0), 1)
        return lax.fori_loop(0, 4, body, jnp.zeros((8, 128), F32))

    def tables():
        pop = popcount_tile((8, 128))
        for layer in range(LAYERS):
            half_angle = jnp.full((8, 128), 0.5, F32) * beta[my_set, layer]

            def entry(q):
                weight = (LOCAL_QUBITS - 2 * q).astype(F32) - 2.0 * pop
                sin_d, cos_d = sincos(half_angle * weight)
                diag[layer, 0, q] = cos_d * (2.0 ** -LOCAL_QUBITS)
                diag[layer, 1, q] = sin_d * (2.0 ** -LOCAL_QUBITS)
                diag[layer, 2, q] = weight
            loop(10, entry)
            sin_h, cos_h = sincos(jnp.concatenate([half_angle, half_angle], axis=0))
            rot[layer + 1, 0] = cos_h
            rot[layer + 1, 1] = sin_h
        rot[0, 0] = jnp.ones((16, 128), F32)
        rot[0, 1] = jnp.zeros((16, 128), F32)
        acc[...] = jnp.zeros((NUM_ACC, 8, 128), F32)

        def init(r):
            rows = pl.ds(pl.multiple_of(r * 16, 16), 16)
            for j in range(4):
                start = jnp.full((16, 256), 2.0 ** -10, F32)
                zero = jnp.zeros((16, 256), F32)
                keep[0, j, rows, :] = start
                keep[1, j, rows, :] = zero
                other[0, 0, j, rows, :] = start
                other[0, 1, j, rows, :] = zero
        loop(16, init)

    def fill(layer, which, half, j):
        def rows_body(r):
            start = pl.multiple_of(r * 32, 32)
            for ct in range(2):
                cost_rows = pl.ds(pl.multiple_of(ct * 256 + start, 32), 32)
                sin_p, cos_p = sincos(gamma[my_set, layer] * cc[which, j, cost_rows, :])
                tab[layer, 0, half * 4 + j, pl.ds(start, 32), cols_of(ct)] = cos_p
                tab[layer, 1, half * 4 + j, pl.ds(start, 32), cols_of(ct)] = sin_p
        loop(8, rows_body)

    def arrive(j):
        cost_arrived(1, j)
        forward_copy(j).start()
        loop(3, lambda n: fill(2 * n, 1, 1, j))
        cost_arrived(0, j)
        loop(LAYERS, lambda n: fill(n, 0, 0, j))
        forward_copy(j).wait()
        loop(2, lambda n: fill(2 * n + 1, 2, 1, j))

    def forward_layer(layer):
        par = lax.rem(layer, 2)

        def alpha(i):
            @pl.when(layer > 0)
            def _():
                exchange(par, i).wait()
                release(i)
            cos_b, sin_b = rot[layer, 0], rot[layer, 1]
            for local_rows, rows, cols, _c in groups(i):
                re, im = [None] * 8, [None] * 8
                for j in range(4):
                    v = rotate(load_state(par, rows, cols, j), cos_b, sin_b)
                    for half in range(2):
                        n = half * 4 + j
                        pr, pi = v[2 * half], v[2 * half + 1]
                        saved[layer, 0, n, rows, cols] = pr
                        saved[layer, 1, n, rows, cols] = pi
                        c, s = tab[layer, 0, n, rows, cols], tab[layer, 1, n, rows, cols]
                        re[n], im[n] = pr * c + pi * s, pi * c - pr * s
                spread(re, im, local_rows, cols)
            right_multiply(state_write(par, i))
        loop(NUM_CHUNKS, alpha)

        @pl.when((layer >= 2))
        def _():
            stash_out(layer - 2).wait()
        middle(layer, par, True)

        @pl.when(layer < 3)
        def _():
            stash_out(layer).start()

        def gamma_sweep(i):
            inverse_chunk(par, i)
            for local_rows, rows, cols, _c in groups(i):
                re, im = gather_big(local_rows, cols)
                for j in range(4):
                    store_state(par, rows, cols, j, (re[j], im[j], re[4 + j], im[4 + j]))

            @pl.when(i > 0)
            def _():
                send(1 - par, i - 1, layer == 0)
        loop(NUM_CHUNKS, gamma_sweep)
        send(1 - par, NUM_CHUNKS - 1, layer == 0)

    def final(i):
        exchange(1, i).wait()
        release(i)
        energy = jnp.zeros((8, 128), F32)
        grad = jnp.zeros((8, 128), F32)
        cos_b, sin_b = rot[LAYERS, 0], rot[LAYERS, 1]
        for local_rows, rows, cols, crows in groups(i):
            for j in range(4):
                kr, ki, orr, oi = rotate(load_state(1, rows, cols, j), cos_b, sin_b)
                ck, co = cc[0, j, crows, :], cc[2, j, crows, :]
                lam = (ck * kr, ck * ki, co * orr, co * oi)
                energy = energy + fold(lam[0] * kr + lam[1] * ki + lam[2] * orr + lam[3] * oi)
                grad = grad + fold((ck - co) * (kr * oi - ki * orr))
                store_state(1, rows, cols, j, rotate(lam, cos_b, -sin_b))
        acc[0] = acc[0] + energy
        acc[2 * LAYERS] = acc[2 * LAYERS] + grad

        @pl.when(i > 0)
        def _():
            send(0, i - 1)

    def backward_layer(step):
        layer = LAYERS - 1 - step
        par = lax.rem(layer, 2)

        def alpha(i):
            exchange(par, i).wait()

            @pl.when(layer > 0)
            def _():
                release(i)
            for local_rows, rows, cols, _c in groups(i):
                v = [load_state(par, rows, cols, j) for j in range(4)]
                re = [v[j][0] for j in range(4)] + [v[j][2] for j in range(4)]
                im = [v[j][1] for j in range(4)] + [v[j][3] for j in range(4)]
                spread(re, im, local_rows, cols)
            right_multiply(state_write(par, i))
        loop(NUM_CHUNKS, alpha)

        @pl.when(layer < 3)
        def _():
            stash_in(layer).wait()
        total = middle(layer, par, False)
        acc[LAYERS + 1 + layer] = acc[LAYERS + 1 + layer] + total

        @pl.when(layer >= 2)
        def _():
            stash_in(layer - 2).start()

        def gamma_sweep(i):
            inverse_chunk(par, i)
            g_sum = jnp.zeros((8, 128), F32)
            b_sum = jnp.zeros((8, 128), F32)
            cos_b, sin_b = rot[layer, 0], rot[layer, 1]
            for local_rows, rows, cols, crows in groups(i):
                re, im = gather_big(local_rows, cols)
                for j in range(4):
                    lam, psi = [], []
                    for half in range(2):
                        n = half * 4 + j
                        c, s = tab[layer, 0, n, rows, cols], tab[layer, 1, n, rows, cols]
                        lr, li = re[n] * c - im[n] * s, im[n] * c + re[n] * s
                        pr, pi = saved[layer, 0, n, rows, cols], saved[layer, 1, n, rows, cols]
                        cost_n = cc[0, j, crows, :] if half == 0 else cc[1 + par, j, crows, :]
                        g_sum = g_sum + fold(cost_n * (lr * pi - li * pr))
                        lam += [lr, li]
                        psi += [pr, pi]
                    b_sum = b_sum + fold(lam[0] * psi[3] - lam[1] * psi[2] + lam[2] * psi[1] - lam[3] * psi[0])
                    store_state(par, rows, cols, j, rotate(lam, cos_b, -sin_b))
            acc[1 + layer] = acc[1 + layer] + 2.0 * g_sum

            @pl.when(layer > 0)
            def _():
                acc[LAYERS + layer] = acc[LAYERS + layer] + b_sum

            @pl.when((i > 0) & (layer > 0))
            def _():
                send(1 - par, i - 1)
        loop(NUM_CHUNKS, gamma_sweep)

        @pl.when(layer > 0)
        def _():
            send(1 - par, NUM_CHUNKS - 1)

    def result_copy(a, b):
        return pltpu.make_async_remote_copy(
            src_ref=mine, dst_ref=res.at[qx], send_sem=r_send.at[a * 4 + b], recv_sem=r_recv.at[qx],
            device_id=(inst, a, b), device_id_type=MESH)

    def others(fn):
        for a in range(4):
            for b in range(4):
                @pl.when((qy != a) | (qx != b))
                def _():
                    fn(result_copy(a, b))

    @pl.when(active)
    def _():
        tables()
        loop(4, arrive)
        loop(LAYERS, forward_layer)
        loop(NUM_CHUNKS, final)
        send(0, NUM_CHUNKS - 1)
        loop(LAYERS, backward_layer)
        mine[...] = jnp.sum(acc[...], axis=1)
        res[qx] = mine[...]
        others(lambda copy: copy.start())

    for slot in range(4):
        @pl.when(jnp.logical_not(active & (qx == slot)))
        def _():
            pltpu.make_async_remote_copy(
                src_ref=mine, dst_ref=res.at[slot], send_sem=r_send.at[0], recv_sem=r_recv.at[slot],
                device_id=partner, device_id_type=MESH).wait_recv()

    for s in range(2):
        total = jnp.sum(res[2 * s] + res[2 * s + 1], axis=1, keepdims=True)
        out[s] = jnp.broadcast_to(total, (NUM_ACC, 128))

    for s in range(2):
        @pl.when(jnp.logical_not(is_self(s)))
        def _():
            cost_copy(s).wait_send()

    @pl.when(active)
    def _():
        others(lambda copy: copy.wait_send())


def hadamard():
    index = jnp.arange(256, dtype=jnp.int32)
    both = index[:, None] & index[None, :]
    parity = jnp.zeros((256, 256), jnp.int32)
    for b in range(8):
        parity = parity ^ ((both >> b) & 1)
    return (1 - 2 * parity).astype(BF16)


def solution(mesh):
    def device_fn(cost, gamma, beta):
        vmem = pltpu.VMEM
        dma = pltpu.SemaphoreType.DMA
        tile = (256, 256)
        out, _ = pl.pallas_call(
            kernel,
            out_shape=(jax.ShapeDtypeStruct((2, NUM_ACC, 128), F32), jax.ShapeDtypeStruct((3, 2, 8) + tile, F32)),
            in_specs=[pl.BlockSpec(memory_space=pl.ANY), pl.BlockSpec(memory_space=pltpu.SMEM),
                      pl.BlockSpec(memory_space=pltpu.SMEM), pl.BlockSpec(memory_space=pltpu.VMEM)],
            out_specs=(pl.BlockSpec(memory_space=pltpu.VMEM), pl.BlockSpec(memory_space=pl.ANY)),
            scratch_shapes=[
                vmem((2, 4) + tile, F32),
                vmem((2, 2, 4) + tile, F32),
                vmem((3, 4, 512, 128), F32),
                vmem((LAYERS, 2, 8) + tile, F32),
                vmem((LAYERS, 2, 8) + tile, F32),
                vmem((2, 2, 8) + tile, F32),
                vmem((LAYERS, 3, 10, 8, 128), F32),
                vmem((LAYERS + 1, 2, 16, 128), F32),
                vmem((NUM_ACC, 8, 128), F32),
                vmem((3, 16, CHUNK, 256), BF16),
                vmem((2,) + tile, F32),
                vmem((16, CHUNK, 256), F32),
                vmem((NUM_ACC, 128), F32),
                vmem((4, NUM_ACC, 128), F32),
                dma((2,)), dma((2, 4)), dma((4,)), dma((4,)), dma((2, NUM_CHUNKS)), dma((2, NUM_CHUNKS)),
                dma((2,)), dma((2,)), dma((16,)), dma((4,)), pltpu.SemaphoreType.REGULAR((NUM_CHUNKS,)),
            ],
            compiler_params=pltpu.CompilerParams(has_side_effects=True, vmem_limit_bytes=67043328),
        )(cost.reshape(512, 128), gamma, beta, hadamard())
        return out[:, 0, 0], out[:, 1:1 + 2 * LAYERS, 0]

    cost_spec = P(('inst', 'qy', 'qx'))
    angle_spec = P('inst', None)
    return jax.shard_map(device_fn, mesh=mesh, in_specs=(cost_spec, angle_spec, angle_spec), out_specs=(P('inst'), angle_spec), check_vma=False)
```

```python
import math
import numpy as np
import jax
import jax.numpy as jnp
from jax import lax
from jax.experimental import pallas as pl
from jax.experimental.pallas import tpu as pltpu
from jax.sharding import PartitionSpec as P

F32 = jnp.float32
BF16 = jnp.bfloat16
LAYERS = 5
LOCAL_QUBITS = 19
CHUNK = 64
STRIP = 64
NUM_CHUNKS = 256 // CHUNK
NUM_ACC = 16
SIN = (3.14159265353629, -5.16771276462444, 2.550163318944362, -0.5992521977957433, 0.08205040168394097, -0.00702838621010907)
COS = (0.9999999997799045, -4.9348021370788056, 4.058709159555753, -1.3352120030448535, 0.23493731379172217, -0.024396324310603436)
MESH = pl.DeviceIdType.MESH
HOMES = ((1, 0), (2, 2))


def sincos_turns(u):
    magic = 12582912.0
    f = u - ((u + magic) - magic)
    z = f * f
    sin_h = f * (SIN[0] + z * (SIN[1] + z * (SIN[2] + z * (SIN[3] + z * (SIN[4] + z * SIN[5])))))
    cos_h = COS[0] + z * (COS[1] + z * (COS[2] + z * (COS[3] + z * (COS[4] + z * COS[5]))))
    twice = sin_h + sin_h
    return twice * cos_h, 1.0 - twice * sin_h


def split3(x):
    a = x.astype(BF16)
    r = x - a.astype(F32)
    b = r.astype(BF16)
    c = (r - b.astype(F32)).astype(BF16)
    return a, b, c


def butterfly8(v):
    for step in (4, 2, 1):
        out = list(v)
        for i in range(8):
            if not i & step:
                out[i] = v[i] + v[i + step]
                out[i + step] = v[i] - v[i + step]
        v = out
    return v


def popcount_tile(shape):
    sub = lax.broadcasted_iota(jnp.int32, shape, 0)
    lane = lax.broadcasted_iota(jnp.int32, shape, 1)
    total = jnp.zeros(shape, jnp.int32)
    for b in range(3):
        total = total + ((sub >> b) & 1)
    for b in range(7):
        total = total + ((lane >> b) & 1)
    return total.astype(F32)


def fold(x):
    return jnp.sum(x.reshape(-1, 8, 128), axis=0)


def cols_of(ct):
    return pl.ds(ct * 128, 128)


def rotate(values, cos_b, sin_b):
    kr, ki, orr, oi = values
    return (cos_b * kr + sin_b * oi, cos_b * ki - sin_b * orr, cos_b * orr + sin_b * ki, cos_b * oi - sin_b * kr)


def groups(i):
    for g in range(CHUNK // 16):
        for ct in range(2):
            start = pl.multiple_of(i * CHUNK + g * 16, 16)
            cost_start = pl.multiple_of(ct * 256 + i * CHUNK + g * 16, 16)
            yield pl.ds(g * 16, 16), pl.ds(start, 16), cols_of(ct), pl.ds(cost_start, 16)


def loop(count, body):
    def step(n, carry):
        body(n)
        return carry
    lax.fori_loop(0, count, step, 0)


def kernel(cost, gamma, beta, had, out, stash, keep, other, cc, tab, saved, hat, diag, rot, acc,
           wide, flip, big, mine, res, c_send, c_recv, f_send, f_recv, x_send, x_recv, h_out, h_in, r_send, r_recv, credit):
    inst = lax.axis_index('inst')
    qy = lax.axis_index('qy')
    qx = lax.axis_index('qx')
    core = lax.rem(qx, 2)
    my_set = qx // 2
    active = qy == my_set + 1
    partner = (inst, qy, qx + 1 - 2 * core)
    kind = lax.rem(qy // 2 + qy, 2)

    def cost_copy(s):
        home_y, home_x = HOMES[s]
        return pltpu.make_async_remote_copy(
            src_ref=cost, dst_ref=cc.at[kind, qx], send_sem=c_send.at[s], recv_sem=c_recv.at[kind, qx],
            device_id=(inst, home_y, home_x + qy // 2), device_id_type=MESH)

    def is_self(s):
        home_y, home_x = HOMES[s]
        return (qy == home_y) & (qx == home_x + qy // 2)

    for s in range(2):
        @pl.when(is_self(s))
        def _():
            pltpu.make_async_copy(cost, cc.at[kind, qx], c_recv.at[kind, qx]).start()

        @pl.when(jnp.logical_not(is_self(s)))
        def _():
            cost_copy(s).start()

    def cost_arrived(which, j):
        pltpu.make_async_copy(cost, cc.at[which, j], c_recv.at[which, j]).wait()

    def forward_copy(j):
        return pltpu.make_async_remote_copy(
            src_ref=cc.at[1, j], dst_ref=cc.at[2, j], send_sem=f_send.at[j], recv_sem=f_recv.at[j],
            device_id=partner, device_id_type=MESH)

    def exchange(parity, i):
        rows = pl.ds(pl.multiple_of(i * CHUNK, CHUNK), CHUNK)
        return pltpu.make_async_remote_copy(
            src_ref=other.at[1 - parity, :, :, rows, :], dst_ref=other.at[parity, :, :, rows, :],
            send_sem=x_send.at[parity, i], recv_sem=x_recv.at[parity, i],
            device_id=partner, device_id_type=MESH)

    def release(i):
        pl.semaphore_signal(credit.at[i], inc=1, device_id=partner, device_id_type=MESH)

    def send(parity, i, first=None):
        if first is None:
            pl.semaphore_wait(credit.at[i], 1)
        else:
            @pl.when(jnp.logical_not(first))
            def _():
                pl.semaphore_wait(credit.at[i], 1)
        exchange(parity, i).start()

    def stash_out(n):
        return pltpu.make_async_copy(hat.at[lax.rem(n, 2)], stash.at[n], h_out.at[lax.rem(n, 2)])

    def stash_in(n):
        return pltpu.make_async_copy(stash.at[n], hat.at[lax.rem(n, 2)], h_in.at[lax.rem(n, 2)])

    def multiply(strips):
        h = had[...]
        for read, write in strips:
            parts = jnp.dot(jnp.concatenate(split3(read()), axis=0), h, preferred_element_type=F32)
            write(parts[0:STRIP] + parts[STRIP:2 * STRIP] + parts[2 * STRIP:3 * STRIP])

    def state_tile(par, t, rows):
        comp, half, j = t // 8, (t // 4) % 2, t % 4
        return keep.at[comp, j, rows, :] if half == 0 else other.at[par, comp, j, rows, :]

    def pair(src, dst):
        def read():
            return src[...]

        def write(value):
            dst[...] = value
        return read, write

    def to_state(par, i):
        rows = pl.ds(pl.multiple_of(i * CHUNK, CHUNK), CHUNK)
        multiply([pair(big.at[t], state_tile(par, t, rows)) for t in range(16)])

    def from_state(par, i):
        rows = pl.ds(pl.multiple_of(i * CHUNK, CHUNK), CHUNK)
        multiply([pair(state_tile(par, t, rows), big.at[t]) for t in range(16)])

    def load_state(par, rows, cols, j):
        return (keep[0, j, rows, cols], keep[1, j, rows, cols],
                other[par, 0, j, rows, cols], other[par, 1, j, rows, cols])

    def store_state(par, rows, cols, j, values):
        keep[0, j, rows, cols] = values[0]
        keep[1, j, rows, cols] = values[1]
        other[par, 0, j, rows, cols] = values[2]
        other[par, 1, j, rows, cols] = values[3]

    def spread(re, im, local_rows, cols):
        for comp, v in enumerate((butterfly8(re), butterfly8(im))):
            for t in range(8):
                big[comp * 8 + t, local_rows, cols] = v[t]

    def gather_big(local_rows, cols):
        re = butterfly8([big[t, local_rows, cols] for t in range(8)])
        im = butterfly8([big[8 + t, local_rows, cols] for t in range(8)])
        return re, im

    def middle(layer, par, forward):
        slot = lax.rem(layer, 2)

        def block(j, total, half):
            n = half * 4 + j
            bits = half + j // 2 + lax.rem(j, 2)
            for comp in range(2):
                src = keep[comp, j] if half == 0 else other[par, comp, j]
                flip[half * 2 + comp] = src.T
            multiply([pair(flip.at[half * 2 + comp, pl.ds(r * STRIP, STRIP), :], wide.at[half * 2 + comp, pl.ds(r * STRIP, STRIP), :])
                      for r in range(256 // STRIP) for comp in range(2)])
            for g in range(16):
                rows = pl.ds(g * 16, 16)
                for ct in range(2):
                    cols = cols_of(ct)
                    q0 = bin(2 * g).count('1') + ct
                    q1 = bin(2 * g + 1).count('1') + ct

                    def pick(m):
                        return jnp.concatenate([diag[layer, m, bits + q0], diag[layer, m, bits + q1]], axis=0)
                    re, im = wide[half * 2, rows, cols], wide[half * 2 + 1, rows, cols]
                    dc, ds = pick(0), pick(1)
                    if forward:
                        re, im = re * dc + im * ds, im * dc - re * ds
                        hat[slot, 0, n, rows, cols] = re
                        hat[slot, 1, n, rows, cols] = im
                    else:
                        term = re * hat[slot, 1, n, rows, cols] - im * hat[slot, 0, n, rows, cols]
                        total = total + fold(term * pick(2))
                        re, im = re * dc - im * ds, im * dc + re * ds
                    wide[half * 2, rows, cols] = re
                    wide[half * 2 + 1, rows, cols] = im
            multiply([pair(wide.at[half * 2 + comp, pl.ds(r * STRIP, STRIP), :], flip.at[half * 2 + comp, pl.ds(r * STRIP, STRIP), :])
                      for r in range(256 // STRIP) for comp in range(2)])
            for comp in range(2):
                value = flip[half * 2 + comp].T
                if half == 0:
                    keep[comp, j] = value
                else:
                    other[par, comp, j] = value
            return total

        def body(j, total):
            return block(j, block(j, total, 0), 1)
        return lax.fori_loop(0, 4, body, jnp.zeros((8, 128), F32))

    def tables():
        pop = popcount_tile((8, 128))
        for layer in range(LAYERS):
            half_angle = jnp.full((8, 128), 0.25 / math.pi, F32) * beta[my_set, layer]

            def entry(q):
                weight = (LOCAL_QUBITS - 2 * q).astype(F32) - 2.0 * pop
                sin_d, cos_d = sincos_turns(half_angle * weight)
                diag[layer, 0, q] = cos_d * (2.0 ** -LOCAL_QUBITS)
                diag[layer, 1, q] = sin_d * (2.0 ** -LOCAL_QUBITS)
                diag[layer, 2, q] = weight
            loop(10, entry)
            sin_h, cos_h = sincos_turns(jnp.concatenate([half_angle, half_angle], axis=0))
            rot[layer + 1, 0] = cos_h
            rot[layer + 1, 1] = sin_h
        rot[0, 0] = jnp.ones((16, 128), F32)
        rot[0, 1] = jnp.zeros((16, 128), F32)
        acc[...] = jnp.zeros((NUM_ACC, 8, 128), F32)

        def init(r):
            rows = pl.ds(pl.multiple_of(r * 16, 16), 16)
            for j in range(4):
                start = jnp.full((16, 256), 2.0 ** -10, F32)
                zero = jnp.zeros((16, 256), F32)
                keep[0, j, rows, :] = start
                keep[1, j, rows, :] = zero
                other[0, 0, j, rows, :] = start
                other[0, 1, j, rows, :] = zero
        loop(16, init)

    def fill(layer, which, half, j):
        turns = gamma[my_set, layer] * (0.5 / math.pi)

        def rows_body(r):
            start = pl.multiple_of(r * 32, 32)
            for ct in range(2):
                cost_rows = pl.ds(pl.multiple_of(ct * 256 + start, 32), 32)
                sin_p, cos_p = sincos_turns(turns * cc[which, j, cost_rows, :])
                tab[layer, 0, half * 4 + j, pl.ds(start, 32), cols_of(ct)] = cos_p
                tab[layer, 1, half * 4 + j, pl.ds(start, 32), cols_of(ct)] = sin_p
        loop(8, rows_body)

    def arrive(j):
        cost_arrived(1, j)
        forward_copy(j).start()
        loop(3, lambda n: fill(2 * n, 1, 1, j))
        cost_arrived(0, j)
        loop(LAYERS, lambda n: fill(n, 0, 0, j))
        forward_copy(j).wait()
        loop(2, lambda n: fill(2 * n + 1, 2, 1, j))

    def forward_layer(layer):
        par = lax.rem(layer, 2)

        def alpha(i):
            @pl.when(layer > 0)
            def _():
                exchange(par, i).wait()
                release(i)
            cos_b, sin_b = rot[layer, 0], rot[layer, 1]
            for local_rows, rows, cols, _c in groups(i):
                re, im = [None] * 8, [None] * 8
                for j in range(4):
                    v = rotate(load_state(par, rows, cols, j), cos_b, sin_b)
                    for half in range(2):
                        n = half * 4 + j
                        pr, pi = v[2 * half], v[2 * half + 1]
                        saved[layer, 0, n, rows, cols] = pr
                        saved[layer, 1, n, rows, cols] = pi
                        c, s = tab[layer, 0, n, rows, cols], tab[layer, 1, n, rows, cols]
                        re[n], im[n] = pr * c + pi * s, pi * c - pr * s
                spread(re, im, local_rows, cols)
            to_state(par, i)
        loop(NUM_CHUNKS, alpha)

        @pl.when((layer >= 2))
        def _():
            stash_out(layer - 2).wait()
        middle(layer, par, True)

        @pl.when(layer < 3)
        def _():
            stash_out(layer).start()

        def gamma_sweep(i):
            from_state(par, i)
            for local_rows, rows, cols, _c in groups(i):
                re, im = gather_big(local_rows, cols)
                for j in range(4):
                    store_state(par, rows, cols, j, (re[j], im[j], re[4 + j], im[4 + j]))

            @pl.when(i > 0)
            def _():
                send(1 - par, i - 1, layer == 0)
        loop(NUM_CHUNKS, gamma_sweep)
        send(1 - par, NUM_CHUNKS - 1, layer == 0)

    def final(i):
        exchange(1, i).wait()
        release(i)
        energy = jnp.zeros((8, 128), F32)
        grad = jnp.zeros((8, 128), F32)
        cos_b, sin_b = rot[LAYERS, 0], rot[LAYERS, 1]
        for local_rows, rows, cols, crows in groups(i):
            for j in range(4):
                kr, ki, orr, oi = rotate(load_state(1, rows, cols, j), cos_b, sin_b)
                ck, co = cc[0, j, crows, :], cc[2, j, crows, :]
                lam = (ck * kr, ck * ki, co * orr, co * oi)
                energy = energy + fold(lam[0] * kr + lam[1] * ki + lam[2] * orr + lam[3] * oi)
                grad = grad + fold((ck - co) * (kr * oi - ki * orr))
                store_state(1, rows, cols, j, rotate(lam, cos_b, -sin_b))
        acc[0] = acc[0] + energy
        acc[2 * LAYERS] = acc[2 * LAYERS] + grad

        @pl.when(i > 0)
        def _():
            send(0, i - 1)

    def backward_layer(step):
        layer = LAYERS - 1 - step
        par = lax.rem(layer, 2)

        def alpha(i):
            exchange(par, i).wait()

            @pl.when(layer > 0)
            def _():
                release(i)
            for local_rows, rows, cols, _c in groups(i):
                v = [load_state(par, rows, cols, j) for j in range(4)]
                re = [v[j][0] for j in range(4)] + [v[j][2] for j in range(4)]
                im = [v[j][1] for j in range(4)] + [v[j][3] for j in range(4)]
                spread(re, im, local_rows, cols)
            to_state(par, i)
        loop(NUM_CHUNKS, alpha)

        @pl.when(layer < 3)
        def _():
            stash_in(layer).wait()
        total = middle(layer, par, False)
        acc[LAYERS + 1 + layer] = acc[LAYERS + 1 + layer] + total

        @pl.when(layer >= 2)
        def _():
            stash_in(layer - 2).start()

        def gamma_sweep(i):
            from_state(par, i)
            g_sum = jnp.zeros((8, 128), F32)
            b_sum = jnp.zeros((8, 128), F32)
            cos_b, sin_b = rot[layer, 0], rot[layer, 1]
            for local_rows, rows, cols, crows in groups(i):
                re, im = gather_big(local_rows, cols)
                for j in range(4):
                    lam, psi = [], []
                    for half in range(2):
                        n = half * 4 + j
                        c, s = tab[layer, 0, n, rows, cols], tab[layer, 1, n, rows, cols]
                        lr, li = re[n] * c - im[n] * s, im[n] * c + re[n] * s
                        pr, pi = saved[layer, 0, n, rows, cols], saved[layer, 1, n, rows, cols]
                        cost_n = cc[0, j, crows, :] if half == 0 else cc[1 + par, j, crows, :]
                        g_sum = g_sum + fold(cost_n * (lr * pi - li * pr))
                        lam += [lr, li]
                        psi += [pr, pi]
                    b_sum = b_sum + fold(lam[0] * psi[3] - lam[1] * psi[2] + lam[2] * psi[1] - lam[3] * psi[0])
                    store_state(par, rows, cols, j, rotate(lam, cos_b, -sin_b))
            acc[1 + layer] = acc[1 + layer] + 2.0 * g_sum

            @pl.when(layer > 0)
            def _():
                acc[LAYERS + layer] = acc[LAYERS + layer] + b_sum

            @pl.when((i > 0) & (layer > 0))
            def _():
                send(1 - par, i - 1)
        loop(NUM_CHUNKS, gamma_sweep)

        @pl.when(layer > 0)
        def _():
            send(1 - par, NUM_CHUNKS - 1)

    def result_copy(a, b):
        return pltpu.make_async_remote_copy(
            src_ref=mine.at[0:NUM_ACC], dst_ref=res.at[qx], send_sem=r_send.at[a * 4 + b], recv_sem=r_recv.at[qx],
            device_id=(inst, a, b), device_id_type=MESH)

    def others(fn):
        for a in range(4):
            for b in range(4):
                @pl.when((qy != a) | (qx != b))
                def _():
                    fn(result_copy(a, b))

    @pl.when(active)
    def _():
        tables()
        loop(4, arrive)
        loop(LAYERS, forward_layer)
        loop(NUM_CHUNKS, final)
        send(0, NUM_CHUNKS - 1)
        loop(LAYERS, backward_layer)
        mine[0:NUM_ACC] = jnp.sum(acc[...], axis=1)
        res[qx] = mine[0:NUM_ACC]
        others(lambda copy: copy.start())

    for slot in range(4):
        @pl.when(jnp.logical_not(active & (qx == slot)))
        def _():
            pltpu.make_async_remote_copy(
                src_ref=mine.at[0:NUM_ACC], dst_ref=res.at[slot], send_sem=r_send.at[0], recv_sem=r_recv.at[slot],
                device_id=partner, device_id_type=MESH).wait_recv()

    for s in range(2):
        total = jnp.sum(res[2 * s] + res[2 * s + 1], axis=1, keepdims=True)
        out[s] = jnp.broadcast_to(total, (NUM_ACC, 128))

    for s in range(2):
        @pl.when(jnp.logical_not(is_self(s)))
        def _():
            cost_copy(s).wait_send()

    @pl.when(active)
    def _():
        others(lambda copy: copy.wait_send())


def hadamard():
    index = jnp.arange(256, dtype=jnp.int32)
    both = index[:, None] & index[None, :]
    parity = jnp.zeros((256, 256), jnp.int32)
    for b in range(8):
        parity = parity ^ ((both >> b) & 1)
    return (1 - 2 * parity).astype(BF16)


def solution(mesh):
    def device_fn(cost, gamma, beta):
        vmem = pltpu.VMEM
        dma = pltpu.SemaphoreType.DMA
        tile = (256, 256)
        out, _ = pl.pallas_call(
            kernel,
            out_shape=(jax.ShapeDtypeStruct((2, NUM_ACC, 128), F32), jax.ShapeDtypeStruct((3, 2, 8) + tile, F32)),
            in_specs=[pl.BlockSpec(memory_space=pl.ANY), pl.BlockSpec(memory_space=pltpu.SMEM),
                      pl.BlockSpec(memory_space=pltpu.SMEM), pl.BlockSpec(memory_space=pltpu.VMEM)],
            out_specs=(pl.BlockSpec(memory_space=pltpu.VMEM), pl.BlockSpec(memory_space=pl.ANY)),
            scratch_shapes=[
                vmem((2, 4) + tile, F32),
                vmem((2, 2, 4) + tile, F32),
                vmem((3, 4, 512, 128), F32),
                vmem((LAYERS, 2, 8) + tile, F32),
                vmem((LAYERS, 2, 8) + tile, F32),
                vmem((2, 2, 8) + tile, F32),
                vmem((LAYERS, 3, 12, 8, 128), F32),
                vmem((LAYERS + 1, 2, 16, 128), F32),
                vmem((NUM_ACC, 8, 128), F32),
                vmem((4,) + tile, F32),
                vmem((4,) + tile, F32),
                vmem((16, CHUNK, 256), F32),
                vmem((2 * NUM_ACC, 128), F32),
                vmem((4, NUM_ACC, 128), F32),
                dma((2,)), dma((2, 4)), dma((4,)), dma((4,)), dma((2, NUM_CHUNKS)), dma((2, NUM_CHUNKS)),
                dma((2,)), dma((2,)), dma((16,)), dma((4,)), pltpu.SemaphoreType.REGULAR((NUM_CHUNKS,)),
            ],
            compiler_params=pltpu.CompilerParams(has_side_effects=True, vmem_limit_bytes=67043328),
        )(cost.reshape(512, 128), gamma, beta, hadamard())
        return out[:, 0, 0], out[:, 1:1 + 2 * LAYERS, 0]

    cost_spec = P(('inst', 'qy', 'qx'))
    angle_spec = P('inst', None)
    return jax.shard_map(device_fn, mesh=mesh, in_specs=(cost_spec, angle_spec, angle_spec), out_specs=(P('inst'), angle_spec), check_vma=False)
```

```python
import math
import numpy as np
import jax
import jax.numpy as jnp
from jax import lax
from jax.experimental import pallas as pl
from jax.experimental.pallas import tpu as pltpu
from jax.sharding import PartitionSpec as P

F32 = jnp.float32
BF16 = jnp.bfloat16
LAYERS = 5
LOCAL_QUBITS = 19
CHUNK = 64
STRIP = 64
NUM_CHUNKS = 256 // CHUNK
NUM_ACC = 16
SIN = (3.14159265353629, -5.16771276462444, 2.550163318944362, -0.5992521977957433, 0.08205040168394097, -0.00702838621010907)
COS = (0.9999999997799045, -4.9348021370788056, 4.058709159555753, -1.3352120030448535, 0.23493731379172217, -0.024396324310603436)
MESH = pl.DeviceIdType.MESH
HOMES = ((1, 0), (2, 2))


def sincos_turns(u):
    magic = 12582912.0
    f = u - ((u + magic) - magic)
    z = f * f
    sin_h = f * (SIN[0] + z * (SIN[1] + z * (SIN[2] + z * (SIN[3] + z * (SIN[4] + z * SIN[5])))))
    cos_h = COS[0] + z * (COS[1] + z * (COS[2] + z * (COS[3] + z * (COS[4] + z * COS[5]))))
    twice = sin_h + sin_h
    return twice * cos_h, 1.0 - twice * sin_h


def split3(x):
    a = x.astype(BF16)
    r = x - a.astype(F32)
    b = r.astype(BF16)
    c = (r - b.astype(F32)).astype(BF16)
    return a, b, c


def butterfly8(v):
    for step in (4, 2, 1):
        out = list(v)
        for i in range(8):
            if not i & step:
                out[i] = v[i] + v[i + step]
                out[i + step] = v[i] - v[i + step]
        v = out
    return v


def popcount_tile(shape):
    sub = lax.broadcasted_iota(jnp.int32, shape, 0)
    lane = lax.broadcasted_iota(jnp.int32, shape, 1)
    total = jnp.zeros(shape, jnp.int32)
    for b in range(3):
        total = total + ((sub >> b) & 1)
    for b in range(7):
        total = total + ((lane >> b) & 1)
    return total.astype(F32)


def fold(x):
    return jnp.sum(x.reshape(-1, 8, 128), axis=0)


def cols_of(ct):
    return pl.ds(ct * 128, 128)


def rotate(values, cos_b, sin_b):
    kr, ki, orr, oi = values
    return (cos_b * kr + sin_b * oi, cos_b * ki - sin_b * orr, cos_b * orr + sin_b * ki, cos_b * oi - sin_b * kr)


def groups(i):
    for g in range(CHUNK // 16):
        for ct in range(2):
            start = pl.multiple_of(i * CHUNK + g * 16, 16)
            cost_start = pl.multiple_of(ct * 256 + i * CHUNK + g * 16, 16)
            yield pl.ds(g * 16, 16), pl.ds(start, 16), cols_of(ct), pl.ds(cost_start, 16)


def loop(count, body):
    def step(n, carry):
        body(n)
        return carry
    lax.fori_loop(0, count, step, 0)


def kernel(cost, gamma, beta, had, out, stash, keep, other, cc, tab, saved, hat, diag, rot, acc,
           wide, flip, big, mine, res, c_send, c_recv, f_send, f_recv, x_send, x_recv, h_out, h_in, r_send, r_recv, relay_send, relay_recv, credit):
    inst = lax.axis_index('inst')
    qy = lax.axis_index('qy')
    qx = lax.axis_index('qx')
    core = lax.rem(qx, 2)
    my_set = qx // 2
    active = qy == my_set + 1
    partner = (inst, qy, qx + 1 - 2 * core)
    kind = lax.rem(qy // 2 + qy, 2)

    def view(s):
        return (qy, qx, qx // 2) if s == 0 else (3 - qy, qx, 1 - qx // 2)

    def home_copy(s, src, origin_y, origin_x, send_sem):
        home_y, home_x = HOMES[s]
        slot = lax.rem(origin_y // 2 + origin_y, 2)
        return pltpu.make_async_remote_copy(
            src_ref=src, dst_ref=cc.at[slot, origin_x], send_sem=send_sem, recv_sem=c_recv.at[slot, origin_x],
            device_id=(inst, home_y, home_x + origin_y // 2), device_id_type=MESH)

    def relay_copy(s, to_y, to_x, r):
        return pltpu.make_async_remote_copy(
            src_ref=cost, dst_ref=cc.at[2, r], send_sem=c_send.at[s], recv_sem=relay_recv.at[r],
            device_id=(inst, to_y, to_x), device_id_type=MESH)

    def is_self(s):
        home_y, home_x = HOMES[s]
        return (qy == home_y) & (qx == home_x + qy // 2)

    def routes(s):
        y, _x, side = view(s)
        near_y = 1 if s == 0 else 2
        corner_y = 0 if s == 0 else 3
        corner_x = qx - 2 if s == 0 else qx + 2
        direct = jnp.logical_not(is_self(s)) & ((side == 0) | (y == 1))
        return [(direct, home_copy(s, cost, qy, qx, c_send.at[s])),
                ((side == 1) & (y == 0), relay_copy(s, corner_y, corner_x, 0)),
                ((side == 1) & (y == 2), relay_copy(s, near_y, qx, 0)),
                ((side == 1) & (y == 3), relay_copy(s, near_y, qx, 1))]

    def relays(s):
        y, _x, side = view(s)
        corner_y = 0 if s == 0 else 3
        corner_x = qx + 2 if s == 0 else qx - 2
        far = (2, 3) if s == 0 else (1, 0)
        out = [((side == 0) & (y == 0), 0, home_copy(s, cc.at[2, 0], corner_y, corner_x, relay_send.at[0]))]
        for r in range(2):
            out.append(((side == 1) & (y == 1), r, home_copy(s, cc.at[2, r], far[r], qx, relay_send.at[r])))
        return out

    def relay_wait(r):
        pltpu.make_async_copy(cost, cc.at[2, r], relay_recv.at[r]).wait()

    for s in range(2):
        @pl.when(is_self(s))
        def _():
            pltpu.make_async_copy(cost, cc.at[kind, qx], c_recv.at[kind, qx]).start()

        for condition, copy in routes(s):
            pl.when(condition)(copy.start)

    for s in range(2):
        for condition, r, copy in relays(s):
            @pl.when(condition)
            def _():
                relay_wait(r)
                copy.start()

    def cost_arrived(which, j):
        pltpu.make_async_copy(cost, cc.at[which, j], c_recv.at[which, j]).wait()

    def forward_copy(j):
        return pltpu.make_async_remote_copy(
            src_ref=cc.at[1, j], dst_ref=cc.at[2, j], send_sem=f_send.at[j], recv_sem=f_recv.at[j],
            device_id=partner, device_id_type=MESH)

    def exchange(parity, i):
        rows = pl.ds(pl.multiple_of(i * CHUNK, CHUNK), CHUNK)
        return pltpu.make_async_remote_copy(
            src_ref=other.at[1 - parity, :, :, rows, :], dst_ref=other.at[parity, :, :, rows, :],
            send_sem=x_send.at[parity, i], recv_sem=x_recv.at[parity, i],
            device_id=partner, device_id_type=MESH)

    def release(i):
        pl.semaphore_signal(credit.at[i], inc=1, device_id=partner, device_id_type=MESH)

    def send(parity, i, first=None):
        if first is None:
            pl.semaphore_wait(credit.at[i], 1)
        else:
            @pl.when(jnp.logical_not(first))
            def _():
                pl.semaphore_wait(credit.at[i], 1)
        exchange(parity, i).start()

    def stash_out(n):
        return pltpu.make_async_copy(hat.at[lax.rem(n, 2)], stash.at[n], h_out.at[lax.rem(n, 2)])

    def stash_in(n):
        return pltpu.make_async_copy(stash.at[n], hat.at[lax.rem(n, 2)], h_in.at[lax.rem(n, 2)])

    def multiply(strips):
        h = had[...]
        for read, write in strips:
            parts = jnp.dot(jnp.concatenate(split3(read()), axis=0), h, preferred_element_type=F32)
            write(parts[0:STRIP] + parts[STRIP:2 * STRIP] + parts[2 * STRIP:3 * STRIP])

    def state_tile(par, t, rows):
        comp, half, j = t // 8, (t // 4) % 2, t % 4
        return keep.at[comp, j, rows, :] if half == 0 else other.at[par, comp, j, rows, :]

    def pair(src, dst):
        def read():
            return src[...]

        def write(value):
            dst[...] = value
        return read, write

    def to_state(par, i):
        rows = pl.ds(pl.multiple_of(i * CHUNK, CHUNK), CHUNK)
        multiply([pair(big.at[t], state_tile(par, t, rows)) for t in range(16)])

    def from_state(par, i):
        rows = pl.ds(pl.multiple_of(i * CHUNK, CHUNK), CHUNK)
        multiply([pair(state_tile(par, t, rows), big.at[t]) for t in range(16)])

    def load_state(par, rows, cols, j):
        return (keep[0, j, rows, cols], keep[1, j, rows, cols],
                other[par, 0, j, rows, cols], other[par, 1, j, rows, cols])

    def store_state(par, rows, cols, j, values):
        keep[0, j, rows, cols] = values[0]
        keep[1, j, rows, cols] = values[1]
        other[par, 0, j, rows, cols] = values[2]
        other[par, 1, j, rows, cols] = values[3]

    def spread(re, im, local_rows, cols):
        for comp, v in enumerate((butterfly8(re), butterfly8(im))):
            for t in range(8):
                big[comp * 8 + t, local_rows, cols] = v[t]

    def gather_big(local_rows, cols):
        re = butterfly8([big[t, local_rows, cols] for t in range(8)])
        im = butterfly8([big[8 + t, local_rows, cols] for t in range(8)])
        return re, im

    def middle(layer, par, forward):
        slot = lax.rem(layer, 2)

        def block(j, total, half):
            n = half * 4 + j
            bits = half + j // 2 + lax.rem(j, 2)
            for comp in range(2):
                src = keep[comp, j] if half == 0 else other[par, comp, j]
                flip[half * 2 + comp] = src.T
            multiply([pair(flip.at[half * 2 + comp, pl.ds(r * STRIP, STRIP), :], wide.at[half * 2 + comp, pl.ds(r * STRIP, STRIP), :])
                      for r in range(256 // STRIP) for comp in range(2)])
            for g in range(16):
                rows = pl.ds(g * 16, 16)
                for ct in range(2):
                    cols = cols_of(ct)
                    q0 = bin(2 * g).count('1') + ct
                    q1 = bin(2 * g + 1).count('1') + ct

                    def pick(m):
                        return jnp.concatenate([diag[layer, m, bits + q0], diag[layer, m, bits + q1]], axis=0)
                    re, im = wide[half * 2, rows, cols], wide[half * 2 + 1, rows, cols]
                    dc, ds = pick(0), pick(1)
                    if forward:
                        re, im = re * dc + im * ds, im * dc - re * ds
                        hat[slot, 0, n, rows, cols] = re
                        hat[slot, 1, n, rows, cols] = im
                    else:
                        term = re * hat[slot, 1, n, rows, cols] - im * hat[slot, 0, n, rows, cols]
                        total = total + fold(term * pick(2))
                        re, im = re * dc - im * ds, im * dc + re * ds
                    wide[half * 2, rows, cols] = re
                    wide[half * 2 + 1, rows, cols] = im
            multiply([pair(wide.at[half * 2 + comp, pl.ds(r * STRIP, STRIP), :], flip.at[half * 2 + comp, pl.ds(r * STRIP, STRIP), :])
                      for r in range(256 // STRIP) for comp in range(2)])
            for comp in range(2):
                value = flip[half * 2 + comp].T
                if half == 0:
                    keep[comp, j] = value
                else:
                    other[par, comp, j] = value
            return total

        def body(j, total):
            return block(j, block(j, total, 0), 1)
        return lax.fori_loop(0, 4, body, jnp.zeros((8, 128), F32))

    def tables():
        pop = popcount_tile((8, 128))
        for layer in range(LAYERS):
            half_angle = jnp.full((8, 128), 0.25 / math.pi, F32) * beta[my_set, layer]

            def entry(q):
                weight = (LOCAL_QUBITS - 2 * q).astype(F32) - 2.0 * pop
                sin_d, cos_d = sincos_turns(half_angle * weight)
                diag[layer, 0, q] = cos_d * (2.0 ** -LOCAL_QUBITS)
                diag[layer, 1, q] = sin_d * (2.0 ** -LOCAL_QUBITS)
                diag[layer, 2, q] = weight
            loop(10, entry)
            sin_h, cos_h = sincos_turns(jnp.concatenate([half_angle, half_angle], axis=0))
            rot[layer + 1, 0] = cos_h
            rot[layer + 1, 1] = sin_h
        rot[0, 0] = jnp.ones((16, 128), F32)
        rot[0, 1] = jnp.zeros((16, 128), F32)
        acc[...] = jnp.zeros((NUM_ACC, 8, 128), F32)

        def init(r):
            rows = pl.ds(pl.multiple_of(r * 16, 16), 16)
            for j in range(4):
                start = jnp.full((16, 256), 2.0 ** -10, F32)
                zero = jnp.zeros((16, 256), F32)
                keep[0, j, rows, :] = start
                keep[1, j, rows, :] = zero
                other[0, 0, j, rows, :] = start
                other[0, 1, j, rows, :] = zero
        loop(16, init)

    def fill(layer, which, half, j):
        turns = gamma[my_set, layer] * (0.5 / math.pi)

        def rows_body(r):
            start = pl.multiple_of(r * 32, 32)
            for ct in range(2):
                cost_rows = pl.ds(pl.multiple_of(ct * 256 + start, 32), 32)
                sin_p, cos_p = sincos_turns(turns * cc[which, j, cost_rows, :])
                tab[layer, 0, half * 4 + j, pl.ds(start, 32), cols_of(ct)] = cos_p
                tab[layer, 1, half * 4 + j, pl.ds(start, 32), cols_of(ct)] = sin_p
        loop(8, rows_body)

    def arrive():
        def own(j):
            cost_arrived(1, j)
            forward_copy(j).start()
            loop(3, lambda n: fill(2 * n, 1, 1, j))

        def passed(j):
            forward_copy(j).wait()
            loop(2, lambda n: fill(2 * n + 1, 2, 1, j))

        def kept(j):
            cost_arrived(0, j)
            loop(LAYERS, lambda n: fill(n, 0, 0, j))
        loop(4, own)
        loop(4, passed)
        loop(4, kept)

    def forward_layer(layer):
        par = lax.rem(layer, 2)

        def alpha(i):
            @pl.when(layer > 0)
            def _():
                exchange(par, i).wait()
                release(i)
            cos_b, sin_b = rot[layer, 0], rot[layer, 1]
            for local_rows, rows, cols, _c in groups(i):
                re, im = [None] * 8, [None] * 8
                for j in range(4):
                    v = rotate(load_state(par, rows, cols, j), cos_b, sin_b)
                    for half in range(2):
                        n = half * 4 + j
                        pr, pi = v[2 * half], v[2 * half + 1]
                        saved[layer, 0, n, rows, cols] = pr
                        saved[layer, 1, n, rows, cols] = pi
                        c, s = tab[layer, 0, n, rows, cols], tab[layer, 1, n, rows, cols]
                        re[n], im[n] = pr * c + pi * s, pi * c - pr * s
                spread(re, im, local_rows, cols)
            to_state(par, i)
        loop(NUM_CHUNKS, alpha)

        @pl.when((layer >= 2))
        def _():
            stash_out(layer - 2).wait()
        middle(layer, par, True)

        @pl.when(layer < 3)
        def _():
            stash_out(layer).start()

        def gamma_sweep(i):
            from_state(par, i)
            for local_rows, rows, cols, _c in groups(i):
                re, im = gather_big(local_rows, cols)
                for j in range(4):
                    store_state(par, rows, cols, j, (re[j], im[j], re[4 + j], im[4 + j]))

            send(1 - par, i, layer == 0)
        loop(NUM_CHUNKS, gamma_sweep)

    def final(i):
        exchange(1, i).wait()
        release(i)
        energy = jnp.zeros((8, 128), F32)
        grad = jnp.zeros((8, 128), F32)
        cos_b, sin_b = rot[LAYERS, 0], rot[LAYERS, 1]
        for local_rows, rows, cols, crows in groups(i):
            for j in range(4):
                kr, ki, orr, oi = rotate(load_state(1, rows, cols, j), cos_b, sin_b)
                ck, co = cc[0, j, crows, :], cc[2, j, crows, :]
                lam = (ck * kr, ck * ki, co * orr, co * oi)
                energy = energy + fold(lam[0] * kr + lam[1] * ki + lam[2] * orr + lam[3] * oi)
                grad = grad + fold((ck - co) * (kr * oi - ki * orr))
                store_state(1, rows, cols, j, rotate(lam, cos_b, -sin_b))
        acc[0] = acc[0] + energy
        acc[2 * LAYERS] = acc[2 * LAYERS] + grad

        send(0, i)

    def backward_layer(step):
        layer = LAYERS - 1 - step
        par = lax.rem(layer, 2)

        def alpha(i):
            exchange(par, i).wait()

            @pl.when(layer > 0)
            def _():
                release(i)
            for local_rows, rows, cols, _c in groups(i):
                v = [load_state(par, rows, cols, j) for j in range(4)]
                re = [v[j][0] for j in range(4)] + [v[j][2] for j in range(4)]
                im = [v[j][1] for j in range(4)] + [v[j][3] for j in range(4)]
                spread(re, im, local_rows, cols)
            to_state(par, i)
        loop(NUM_CHUNKS, alpha)

        @pl.when(layer < 3)
        def _():
            stash_in(layer).wait()
        total = middle(layer, par, False)
        acc[LAYERS + 1 + layer] = acc[LAYERS + 1 + layer] + total

        @pl.when(layer >= 2)
        def _():
            stash_in(layer - 2).start()

        def gamma_sweep(i):
            from_state(par, i)
            g_sum = jnp.zeros((8, 128), F32)
            b_sum = jnp.zeros((8, 128), F32)
            cos_b, sin_b = rot[layer, 0], rot[layer, 1]
            for local_rows, rows, cols, crows in groups(i):
                re, im = gather_big(local_rows, cols)
                for j in range(4):
                    lam, psi = [], []
                    for half in range(2):
                        n = half * 4 + j
                        c, s = tab[layer, 0, n, rows, cols], tab[layer, 1, n, rows, cols]
                        lr, li = re[n] * c - im[n] * s, im[n] * c + re[n] * s
                        pr, pi = saved[layer, 0, n, rows, cols], saved[layer, 1, n, rows, cols]
                        cost_n = cc[0, j, crows, :] if half == 0 else cc[1 + par, j, crows, :]
                        g_sum = g_sum + fold(cost_n * (lr * pi - li * pr))
                        lam += [lr, li]
                        psi += [pr, pi]
                    b_sum = b_sum + fold(lam[0] * psi[3] - lam[1] * psi[2] + lam[2] * psi[1] - lam[3] * psi[0])
                    store_state(par, rows, cols, j, rotate(lam, cos_b, -sin_b))
            acc[1 + layer] = acc[1 + layer] + 2.0 * g_sum

            @pl.when(layer > 0)
            def _():
                acc[LAYERS + layer] = acc[LAYERS + layer] + b_sum

            @pl.when(layer > 0)
            def _():
                send(1 - par, i)
        loop(NUM_CHUNKS, gamma_sweep)

    def result_copy(a, b):
        return pltpu.make_async_remote_copy(
            src_ref=mine.at[0:NUM_ACC], dst_ref=res.at[qx], send_sem=r_send.at[a * 4 + b], recv_sem=r_recv.at[qx],
            device_id=(inst, a, b), device_id_type=MESH)

    def others(fn):
        for a in range(4):
            for b in range(4):
                @pl.when((qy != a) | (qx != b))
                def _():
                    fn(result_copy(a, b))

    @pl.when(active)
    def _():
        tables()
        arrive()
        loop(LAYERS, forward_layer)
        loop(NUM_CHUNKS, final)
        loop(LAYERS, backward_layer)
        mine[0:NUM_ACC] = jnp.sum(acc[...], axis=1)
        res[qx] = mine[0:NUM_ACC]
        others(lambda copy: copy.start())

    for slot in range(4):
        @pl.when(jnp.logical_not(active & (qx == slot)))
        def _():
            pltpu.make_async_remote_copy(
                src_ref=mine.at[0:NUM_ACC], dst_ref=res.at[slot], send_sem=r_send.at[0], recv_sem=r_recv.at[slot],
                device_id=partner, device_id_type=MESH).wait_recv()

    for s in range(2):
        total = jnp.sum(res[2 * s] + res[2 * s + 1], axis=1, keepdims=True)
        out[s] = jnp.broadcast_to(total, (NUM_ACC, 128))

    for s in range(2):
        @pl.when(jnp.logical_not(is_self(s)))
        def _():
            home_copy(s, cost, qy, qx, c_send.at[s]).wait_send()

        for condition, r, copy in relays(s):
            pl.when(condition)(copy.wait_send)

    @pl.when(active)
    def _():
        others(lambda copy: copy.wait_send())


def hadamard():
    index = np.arange(256)
    both = index[:, None] & index[None, :]
    parity = sum((both >> b) & 1 for b in range(8)) & 1
    return jnp.asarray(1.0 - 2.0 * parity, BF16)


def solution(mesh):
    def device_fn(cost, gamma, beta):
        vmem = pltpu.VMEM
        dma = pltpu.SemaphoreType.DMA
        tile = (256, 256)
        out, _ = pl.pallas_call(
            kernel,
            out_shape=(jax.ShapeDtypeStruct((2, NUM_ACC, 128), F32), jax.ShapeDtypeStruct((3, 2, 8) + tile, F32)),
            in_specs=[pl.BlockSpec(memory_space=pl.ANY), pl.BlockSpec(memory_space=pltpu.SMEM),
                      pl.BlockSpec(memory_space=pltpu.SMEM), pl.BlockSpec(memory_space=pltpu.VMEM)],
            out_specs=(pl.BlockSpec(memory_space=pltpu.VMEM), pl.BlockSpec(memory_space=pl.ANY)),
            scratch_shapes=[
                vmem((2, 4) + tile, F32),
                vmem((2, 2, 4) + tile, F32),
                vmem((3, 4, 512, 128), F32),
                vmem((LAYERS, 2, 8) + tile, F32),
                vmem((LAYERS, 2, 8) + tile, F32),
                vmem((2, 2, 8) + tile, F32),
                vmem((LAYERS, 3, 12, 8, 128), F32),
                vmem((LAYERS + 1, 2, 16, 128), F32),
                vmem((NUM_ACC, 8, 128), F32),
                vmem((4,) + tile, F32),
                vmem((4,) + tile, F32),
                vmem((16, CHUNK, 256), F32),
                vmem((2 * NUM_ACC, 128), F32),
                vmem((4, NUM_ACC, 128), F32),
                dma((2,)), dma((2, 4)), dma((4,)), dma((4,)), dma((2, NUM_CHUNKS)), dma((2, NUM_CHUNKS)),
                dma((2,)), dma((2,)), dma((16,)), dma((4,)), dma((2,)), dma((2,)), pltpu.SemaphoreType.REGULAR((NUM_CHUNKS,)),
            ],
            compiler_params=pltpu.CompilerParams(has_side_effects=True, vmem_limit_bytes=67043328),
        )(cost.reshape(512, 128), gamma, beta, hadamard())
        return out[:, 0, 0], out[:, 1:1 + 2 * LAYERS, 0]

    cost_spec = P(('inst', 'qy', 'qx'))
    angle_spec = P('inst', None)
    return jax.shard_map(device_fn, mesh=mesh, in_specs=(cost_spec, angle_spec, angle_spec), out_specs=(P('inst'), angle_spec), check_vma=False)
```

```python
import math
import numpy as np
import jax
import jax.numpy as jnp
from jax import lax
from jax.experimental import pallas as pl
from jax.experimental.pallas import tpu as pltpu
from jax.sharding import PartitionSpec as P

F32 = jnp.float32
BF16 = jnp.bfloat16
LAYERS = 5
LOCAL_QUBITS = 19
CHUNK = 64
STRIP = 64
NUM_CHUNKS = 256 // CHUNK
NUM_ACC = 16
SIN = (3.14159265353629, -5.16771276462444, 2.550163318944362, -0.5992521977957433, 0.08205040168394097, -0.00702838621010907)
COS = (0.9999999997799045, -4.9348021370788056, 4.058709159555753, -1.3352120030448535, 0.23493731379172217, -0.024396324310603436)
MESH = pl.DeviceIdType.MESH
PARTS = tuple(pl.ds(n * 64, 64) for n in range(8))
HOMES = ((1, 0), (2, 2))


def sincos_turns(u):
    magic = 12582912.0
    f = u - ((u + magic) - magic)
    z = f * f
    sin_h = f * (SIN[0] + z * (SIN[1] + z * (SIN[2] + z * (SIN[3] + z * (SIN[4] + z * SIN[5])))))
    cos_h = COS[0] + z * (COS[1] + z * (COS[2] + z * (COS[3] + z * (COS[4] + z * COS[5]))))
    twice = sin_h + sin_h
    return twice * cos_h, 1.0 - twice * sin_h


def split3(x):
    a = x.astype(BF16)
    r = x - a.astype(F32)
    b = r.astype(BF16)
    c = (r - b.astype(F32)).astype(BF16)
    return a, b, c


def butterfly8(v):
    for step in (4, 2, 1):
        out = list(v)
        for i in range(8):
            if not i & step:
                out[i] = v[i] + v[i + step]
                out[i + step] = v[i] - v[i + step]
        v = out
    return v


def popcount_tile(shape):
    sub = lax.broadcasted_iota(jnp.int32, shape, 0)
    lane = lax.broadcasted_iota(jnp.int32, shape, 1)
    total = jnp.zeros(shape, jnp.int32)
    for b in range(3):
        total = total + ((sub >> b) & 1)
    for b in range(7):
        total = total + ((lane >> b) & 1)
    return total.astype(F32)


def fold(x):
    return jnp.sum(x.reshape(-1, 8, 128), axis=0)


def cols_of(ct):
    return pl.ds(ct * 128, 128)


def rotate(values, cos_b, sin_b):
    kr, ki, orr, oi = values
    return (cos_b * kr + sin_b * oi, cos_b * ki - sin_b * orr, cos_b * orr + sin_b * ki, cos_b * oi - sin_b * kr)


def groups(i):
    for g in range(CHUNK // 16):
        for ct in range(2):
            start = pl.multiple_of(i * CHUNK + g * 16, 16)
            cost_start = pl.multiple_of(ct * 256 + i * CHUNK + g * 16, 16)
            yield pl.ds(g * 16, 16), pl.ds(start, 16), cols_of(ct), pl.ds(cost_start, 16)


def loop(count, body):
    def step(n, carry):
        body(n)
        return carry
    lax.fori_loop(0, count, step, 0)


def kernel(cost, gamma, beta, had, out, stash, keep, other, cc, tab, saved, hat, diag, rot, acc,
           wide, flip, big, mine, res, c_send, c_recv, f_send, f_recv, x_send, x_recv, h_out, h_in, r_send, r_recv, relay_send, relay_recv, credit):
    inst = lax.axis_index('inst')
    qy = lax.axis_index('qy')
    qx = lax.axis_index('qx')
    core = lax.rem(qx, 2)
    my_set = qx // 2
    active = qy == my_set + 1
    partner = (inst, qy, qx + 1 - 2 * core)
    kind = lax.rem(qy // 2 + qy, 2)

    def view(s):
        return (qy, qx, qx // 2) if s == 0 else (3 - qy, qx, 1 - qx // 2)

    def home_copy(s, src, origin_y, origin_x, send_sem, part=None):
        home_y, home_x = HOMES[s]
        slot = lax.rem(origin_y // 2 + origin_y, 2)
        dst = cc.at[slot, origin_x]
        if part is not None:
            src, dst = src.at[part], dst.at[part]
        return pltpu.make_async_remote_copy(
            src_ref=src, dst_ref=dst, send_sem=send_sem, recv_sem=c_recv.at[slot, origin_x],
            device_id=(inst, home_y, home_x + origin_y // 2), device_id_type=MESH)

    def relay_copies(s, to_y, to_x, r):
        return [pltpu.make_async_remote_copy(
            src_ref=cost.at[part], dst_ref=cc.at[2, r].at[part], send_sem=c_send.at[s], recv_sem=relay_recv.at[r, n],
            device_id=(inst, to_y, to_x), device_id_type=MESH) for n, part in enumerate(PARTS)]

    def is_self(s):
        home_y, home_x = HOMES[s]
        return (qy == home_y) & (qx == home_x + qy // 2)

    def routes(s):
        y, _x, side = view(s)
        near_y = 1 if s == 0 else 2
        corner_y = 0 if s == 0 else 3
        corner_x = qx - 2 if s == 0 else qx + 2
        direct = jnp.logical_not(is_self(s)) & ((side == 0) | (y == 1))
        return [(direct, [home_copy(s, cost, qy, qx, c_send.at[s])]),
                ((side == 1) & (y == 0), relay_copies(s, corner_y, corner_x, 0)),
                ((side == 1) & (y == 2), relay_copies(s, near_y, qx, 0)),
                ((side == 1) & (y == 3), relay_copies(s, near_y, qx, 1))]

    def relays(s):
        y, _x, side = view(s)
        corner_y = 0 if s == 0 else 3
        corner_x = qx + 2 if s == 0 else qx - 2
        far = (2, 3) if s == 0 else (1, 0)
        return [((side == 0) & (y == 0), [(0, corner_y, corner_x)]),
                ((side == 1) & (y == 1), [(r, far[r], qx) for r in range(2)])]

    for s in range(2):
        @pl.when(is_self(s))
        def _():
            pltpu.make_async_copy(cost, cc.at[kind, qx], c_recv.at[kind, qx]).start()

        for condition, copies in routes(s):
            @pl.when(condition)
            def _():
                for copy in copies:
                    copy.start()

    for s in range(2):
        for condition, blocks in relays(s):
            @pl.when(condition)
            def _():
                for n, part in enumerate(PARTS):
                    for r, origin_y, origin_x in blocks:
                        pltpu.make_async_copy(cost.at[part], cc.at[2, r].at[part], relay_recv.at[r, n]).wait()
                        home_copy(s, cc.at[2, r], origin_y, origin_x, relay_send.at[r], part).start()

    def cost_arrived(which, j):
        pltpu.make_async_copy(cost, cc.at[which, j], c_recv.at[which, j]).wait()

    def forward_copy(j):
        return pltpu.make_async_remote_copy(
            src_ref=cc.at[1, j], dst_ref=cc.at[2, j], send_sem=f_send.at[j], recv_sem=f_recv.at[j],
            device_id=partner, device_id_type=MESH)

    def exchange(parity, i):
        rows = pl.ds(pl.multiple_of(i * CHUNK, CHUNK), CHUNK)
        return pltpu.make_async_remote_copy(
            src_ref=other.at[1 - parity, :, :, rows, :], dst_ref=other.at[parity, :, :, rows, :],
            send_sem=x_send.at[parity, i], recv_sem=x_recv.at[parity, i],
            device_id=partner, device_id_type=MESH)

    def release(i):
        pl.semaphore_signal(credit.at[i], inc=1, device_id=partner, device_id_type=MESH)

    def send(parity, i, first=None):
        if first is None:
            pl.semaphore_wait(credit.at[i], 1)
        else:
            @pl.when(jnp.logical_not(first))
            def _():
                pl.semaphore_wait(credit.at[i], 1)
        exchange(parity, i).start()

    def stash_out(n):
        return pltpu.make_async_copy(hat.at[lax.rem(n, 2)], stash.at[n], h_out.at[lax.rem(n, 2)])

    def stash_in(n):
        return pltpu.make_async_copy(stash.at[n], hat.at[lax.rem(n, 2)], h_in.at[lax.rem(n, 2)])

    def multiply(strips):
        h = had[...]
        for read, write in strips:
            parts = jnp.dot(jnp.concatenate(split3(read()), axis=0), h, preferred_element_type=F32)
            write(parts[0:STRIP] + parts[STRIP:2 * STRIP] + parts[2 * STRIP:3 * STRIP])

    def state_tile(par, t, rows):
        comp, half, j = t // 8, (t // 4) % 2, t % 4
        return keep.at[comp, j, rows, :] if half == 0 else other.at[par, comp, j, rows, :]

    def pair(src, dst):
        def read():
            return src[...]

        def write(value):
            dst[...] = value
        return read, write

    def to_state(par, i):
        rows = pl.ds(pl.multiple_of(i * CHUNK, CHUNK), CHUNK)
        multiply([pair(big.at[t], state_tile(par, t, rows)) for t in range(16)])

    def from_state(par, i):
        rows = pl.ds(pl.multiple_of(i * CHUNK, CHUNK), CHUNK)
        multiply([pair(state_tile(par, t, rows), big.at[t]) for t in range(16)])

    def load_state(par, rows, cols, j):
        return (keep[0, j, rows, cols], keep[1, j, rows, cols],
                other[par, 0, j, rows, cols], other[par, 1, j, rows, cols])

    def store_state(par, rows, cols, j, values):
        keep[0, j, rows, cols] = values[0]
        keep[1, j, rows, cols] = values[1]
        other[par, 0, j, rows, cols] = values[2]
        other[par, 1, j, rows, cols] = values[3]

    def spread(re, im, local_rows, cols):
        for comp, v in enumerate((butterfly8(re), butterfly8(im))):
            for t in range(8):
                big[comp * 8 + t, local_rows, cols] = v[t]

    def gather_big(local_rows, cols):
        re = butterfly8([big[t, local_rows, cols] for t in range(8)])
        im = butterfly8([big[8 + t, local_rows, cols] for t in range(8)])
        return re, im

    def middle(layer, par, forward):
        slot = lax.rem(layer, 2)

        def block(j, total, half):
            n = half * 4 + j
            bits = half + j // 2 + lax.rem(j, 2)
            for comp in range(2):
                src = keep[comp, j] if half == 0 else other[par, comp, j]
                flip[half * 2 + comp] = src.T
            multiply([pair(flip.at[half * 2 + comp, pl.ds(r * STRIP, STRIP), :], wide.at[half * 2 + comp, pl.ds(r * STRIP, STRIP), :])
                      for r in range(256 // STRIP) for comp in range(2)])
            for g in range(16):
                rows = pl.ds(g * 16, 16)
                for ct in range(2):
                    cols = cols_of(ct)
                    q0 = bin(2 * g).count('1') + ct
                    q1 = bin(2 * g + 1).count('1') + ct

                    def pick(m):
                        return jnp.concatenate([diag[layer, m, bits + q0], diag[layer, m, bits + q1]], axis=0)
                    re, im = wide[half * 2, rows, cols], wide[half * 2 + 1, rows, cols]
                    dc, ds = pick(0), pick(1)
                    if forward:
                        re, im = re * dc + im * ds, im * dc - re * ds
                        hat[slot, 0, n, rows, cols] = re
                        hat[slot, 1, n, rows, cols] = im
                    else:
                        term = re * hat[slot, 1, n, rows, cols] - im * hat[slot, 0, n, rows, cols]
                        total = total + fold(term * pick(2))
                        re, im = re * dc - im * ds, im * dc + re * ds
                    wide[half * 2, rows, cols] = re
                    wide[half * 2 + 1, rows, cols] = im
            multiply([pair(wide.at[half * 2 + comp, pl.ds(r * STRIP, STRIP), :], flip.at[half * 2 + comp, pl.ds(r * STRIP, STRIP), :])
                      for r in range(256 // STRIP) for comp in range(2)])
            for comp in range(2):
                value = flip[half * 2 + comp].T
                if half == 0:
                    keep[comp, j] = value
                else:
                    other[par, comp, j] = value
            return total

        def body(j, total):
            return block(j, block(j, total, 0), 1)
        return lax.fori_loop(0, 4, body, jnp.zeros((8, 128), F32))

    def tables():
        pop = popcount_tile((8, 128))
        for layer in range(LAYERS):
            half_angle = jnp.full((8, 128), 0.25 / math.pi, F32) * beta[my_set, layer]

            def entry(q):
                weight = (LOCAL_QUBITS - 2 * q).astype(F32) - 2.0 * pop
                sin_d, cos_d = sincos_turns(half_angle * weight)
                diag[layer, 0, q] = cos_d * (2.0 ** -LOCAL_QUBITS)
                diag[layer, 1, q] = sin_d * (2.0 ** -LOCAL_QUBITS)
                diag[layer, 2, q] = weight
            loop(10, entry)
            sin_h, cos_h = sincos_turns(jnp.concatenate([half_angle, half_angle], axis=0))
            rot[layer + 1, 0] = cos_h
            rot[layer + 1, 1] = sin_h
        rot[0, 0] = jnp.ones((16, 128), F32)
        rot[0, 1] = jnp.zeros((16, 128), F32)
        acc[...] = jnp.zeros((NUM_ACC, 8, 128), F32)

        def init(r):
            rows = pl.ds(pl.multiple_of(r * 16, 16), 16)
            for j in range(4):
                start = jnp.full((16, 256), 2.0 ** -10, F32)
                zero = jnp.zeros((16, 256), F32)
                keep[0, j, rows, :] = start
                keep[1, j, rows, :] = zero
                other[0, 0, j, rows, :] = start
                other[0, 1, j, rows, :] = zero
        loop(16, init)

    def fill(layer, which, half, j):
        turns = gamma[my_set, layer] * (0.5 / math.pi)

        def rows_body(r):
            start = pl.multiple_of(r * 32, 32)
            for ct in range(2):
                cost_rows = pl.ds(pl.multiple_of(ct * 256 + start, 32), 32)
                sin_p, cos_p = sincos_turns(turns * cc[which, j, cost_rows, :])
                tab[layer, 0, half * 4 + j, pl.ds(start, 32), cols_of(ct)] = cos_p
                tab[layer, 1, half * 4 + j, pl.ds(start, 32), cols_of(ct)] = sin_p
        loop(8, rows_body)

    def arrive():
        def own(j):
            cost_arrived(1, j)
            forward_copy(j).start()
            loop(3, lambda n: fill(2 * n, 1, 1, j))

        def passed(j):
            forward_copy(j).wait()
            loop(2, lambda n: fill(2 * n + 1, 2, 1, j))

        def kept(j):
            cost_arrived(0, j)
            loop(LAYERS, lambda n: fill(n, 0, 0, j))
        def near_then_far(step):
            near = lax.rem(step + my_set, 2) * 2
            loop(2, lambda n: own(near + n))

            @pl.when(step == 1)
            def _():
                loop(4, passed)
            loop(2, lambda n: kept(near + n))
        loop(2, near_then_far)

    def forward_layer(layer):
        par = lax.rem(layer, 2)

        def alpha(i):
            @pl.when(layer > 0)
            def _():
                exchange(par, i).wait()
                release(i)
            cos_b, sin_b = rot[layer, 0], rot[layer, 1]
            for local_rows, rows, cols, _c in groups(i):
                re, im = [None] * 8, [None] * 8
                for j in range(4):
                    v = rotate(load_state(par, rows, cols, j), cos_b, sin_b)
                    for half in range(2):
                        n = half * 4 + j
                        pr, pi = v[2 * half], v[2 * half + 1]
                        saved[layer, 0, n, rows, cols] = pr
                        saved[layer, 1, n, rows, cols] = pi
                        c, s = tab[layer, 0, n, rows, cols], tab[layer, 1, n, rows, cols]
                        re[n], im[n] = pr * c + pi * s, pi * c - pr * s
                spread(re, im, local_rows, cols)
            to_state(par, i)
        loop(NUM_CHUNKS, alpha)

        @pl.when((layer >= 2))
        def _():
            stash_out(layer - 2).wait()
        middle(layer, par, True)

        @pl.when(layer < 3)
        def _():
            stash_out(layer).start()

        def gamma_sweep(i):
            from_state(par, i)
            for local_rows, rows, cols, _c in groups(i):
                re, im = gather_big(local_rows, cols)
                for j in range(4):
                    store_state(par, rows, cols, j, (re[j], im[j], re[4 + j], im[4 + j]))

            send(1 - par, i, layer == 0)
        loop(NUM_CHUNKS, gamma_sweep)

    def final(i):
        exchange(1, i).wait()
        release(i)
        energy = jnp.zeros((8, 128), F32)
        grad = jnp.zeros((8, 128), F32)
        cos_b, sin_b = rot[LAYERS, 0], rot[LAYERS, 1]
        for local_rows, rows, cols, crows in groups(i):
            for j in range(4):
                kr, ki, orr, oi = rotate(load_state(1, rows, cols, j), cos_b, sin_b)
                ck, co = cc[0, j, crows, :], cc[2, j, crows, :]
                lam = (ck * kr, ck * ki, co * orr, co * oi)
                energy = energy + fold(lam[0] * kr + lam[1] * ki + lam[2] * orr + lam[3] * oi)
                grad = grad + fold((ck - co) * (kr * oi - ki * orr))
                store_state(1, rows, cols, j, rotate(lam, cos_b, -sin_b))
        acc[0] = acc[0] + energy
        acc[2 * LAYERS] = acc[2 * LAYERS] + grad

        send(0, i)

    def backward_layer(step):
        layer = LAYERS - 1 - step
        par = lax.rem(layer, 2)

        def alpha(i):
            exchange(par, i).wait()

            @pl.when(layer > 0)
            def _():
                release(i)
            for local_rows, rows, cols, _c in groups(i):
                v = [load_state(par, rows, cols, j) for j in range(4)]
                re = [v[j][0] for j in range(4)] + [v[j][2] for j in range(4)]
                im = [v[j][1] for j in range(4)] + [v[j][3] for j in range(4)]
                spread(re, im, local_rows, cols)
            to_state(par, i)
        loop(NUM_CHUNKS, alpha)

        @pl.when(layer < 3)
        def _():
            stash_in(layer).wait()
        total = middle(layer, par, False)
        acc[LAYERS + 1 + layer] = acc[LAYERS + 1 + layer] + total

        @pl.when(layer >= 2)
        def _():
            stash_in(layer - 2).start()

        def gamma_sweep(i):
            from_state(par, i)
            g_sum = jnp.zeros((8, 128), F32)
            b_sum = jnp.zeros((8, 128), F32)
            cos_b, sin_b = rot[layer, 0], rot[layer, 1]
            for local_rows, rows, cols, crows in groups(i):
                re, im = gather_big(local_rows, cols)
                for j in range(4):
                    lam, psi = [], []
                    for half in range(2):
                        n = half * 4 + j
                        c, s = tab[layer, 0, n, rows, cols], tab[layer, 1, n, rows, cols]
                        lr, li = re[n] * c - im[n] * s, im[n] * c + re[n] * s
                        pr, pi = saved[layer, 0, n, rows, cols], saved[layer, 1, n, rows, cols]
                        cost_n = cc[0, j, crows, :] if half == 0 else cc[1 + par, j, crows, :]
                        g_sum = g_sum + fold(cost_n * (lr * pi - li * pr))
                        lam += [lr, li]
                        psi += [pr, pi]
                    b_sum = b_sum + fold(lam[0] * psi[3] - lam[1] * psi[2] + lam[2] * psi[1] - lam[3] * psi[0])
                    store_state(par, rows, cols, j, rotate(lam, cos_b, -sin_b))
            acc[1 + layer] = acc[1 + layer] + 2.0 * g_sum

            @pl.when(layer > 0)
            def _():
                acc[LAYERS + layer] = acc[LAYERS + layer] + b_sum

            @pl.when(layer > 0)
            def _():
                send(1 - par, i)
        loop(NUM_CHUNKS, gamma_sweep)

    def result_copy(a, b):
        return pltpu.make_async_remote_copy(
            src_ref=mine.at[0:NUM_ACC], dst_ref=res.at[qx], send_sem=r_send.at[a * 4 + b], recv_sem=r_recv.at[qx],
            device_id=(inst, a, b), device_id_type=MESH)

    def others(fn):
        for a in range(4):
            for b in range(4):
                @pl.when((qy != a) | (qx != b))
                def _():
                    fn(result_copy(a, b))

    @pl.when(active)
    def _():
        tables()
        arrive()
        loop(LAYERS, forward_layer)
        loop(NUM_CHUNKS, final)
        loop(LAYERS, backward_layer)
        mine[0:NUM_ACC] = jnp.sum(acc[...], axis=1)
        res[qx] = mine[0:NUM_ACC]
        others(lambda copy: copy.start())

    for slot in range(4):
        @pl.when(jnp.logical_not(active & (qx == slot)))
        def _():
            pltpu.make_async_remote_copy(
                src_ref=mine.at[0:NUM_ACC], dst_ref=res.at[slot], send_sem=r_send.at[0], recv_sem=r_recv.at[slot],
                device_id=partner, device_id_type=MESH).wait_recv()

    for s in range(2):
        total = jnp.sum(res[2 * s] + res[2 * s + 1], axis=1, keepdims=True)
        out[s] = jnp.broadcast_to(total, (NUM_ACC, 128))

    for s in range(2):
        @pl.when(jnp.logical_not(is_self(s)))
        def _():
            home_copy(s, cost, qy, qx, c_send.at[s]).wait_send()

        for condition, blocks in relays(s):
            @pl.when(condition)
            def _():
                for r, origin_y, origin_x in blocks:
                    home_copy(s, cc.at[2, r], origin_y, origin_x, relay_send.at[r]).wait_send()

    @pl.when(active)
    def _():
        others(lambda copy: copy.wait_send())


def hadamard():
    index = np.arange(256)
    both = index[:, None] & index[None, :]
    parity = sum((both >> b) & 1 for b in range(8)) & 1
    return jnp.asarray(1.0 - 2.0 * parity, BF16)


def solution(mesh):
    def device_fn(cost, gamma, beta):
        vmem = pltpu.VMEM
        dma = pltpu.SemaphoreType.DMA
        tile = (256, 256)
        out, _ = pl.pallas_call(
            kernel,
            out_shape=(jax.ShapeDtypeStruct((2, NUM_ACC, 128), F32), jax.ShapeDtypeStruct((3, 2, 8) + tile, F32)),
            in_specs=[pl.BlockSpec(memory_space=pl.ANY), pl.BlockSpec(memory_space=pltpu.SMEM),
                      pl.BlockSpec(memory_space=pltpu.SMEM), pl.BlockSpec(memory_space=pltpu.VMEM)],
            out_specs=(pl.BlockSpec(memory_space=pltpu.VMEM), pl.BlockSpec(memory_space=pl.ANY)),
            scratch_shapes=[
                vmem((2, 4) + tile, F32),
                vmem((2, 2, 4) + tile, F32),
                vmem((3, 4, 512, 128), F32),
                vmem((LAYERS, 2, 8) + tile, F32),
                vmem((LAYERS, 2, 8) + tile, F32),
                vmem((2, 2, 8) + tile, F32),
                vmem((LAYERS, 3, 12, 8, 128), F32),
                vmem((LAYERS + 1, 2, 16, 128), F32),
                vmem((NUM_ACC, 8, 128), F32),
                vmem((4,) + tile, F32),
                vmem((4,) + tile, F32),
                vmem((16, CHUNK, 256), F32),
                vmem((2 * NUM_ACC, 128), F32),
                vmem((4, NUM_ACC, 128), F32),
                dma((2,)), dma((2, 4)), dma((4,)), dma((4,)), dma((2, NUM_CHUNKS)), dma((2, NUM_CHUNKS)),
                dma((2,)), dma((2,)), dma((16,)), dma((4,)), dma((2,)), dma((2, len(PARTS))), pltpu.SemaphoreType.REGULAR((NUM_CHUNKS,)),
            ],
            compiler_params=pltpu.CompilerParams(has_side_effects=True, vmem_limit_bytes=67043328),
        )(cost.reshape(512, 128), gamma, beta, hadamard())
        return out[:, 0, 0], out[:, 1:1 + 2 * LAYERS, 0]

    cost_spec = P(('inst', 'qy', 'qx'))
    angle_spec = P('inst', None)
    return jax.shard_map(device_fn, mesh=mesh, in_specs=(cost_spec, angle_spec, angle_spec), out_specs=(P('inst'), angle_spec), check_vma=False)
```

```python
import math
import numpy as np
import jax
import jax.numpy as jnp
from jax import lax
from jax.experimental import pallas as pl
from jax.experimental.pallas import tpu as pltpu
from jax.sharding import PartitionSpec as P

F32 = jnp.float32
BF16 = jnp.bfloat16
LAYERS = 5
LOCAL_QUBITS = 19
CHUNK = 64
STRIP = 64
NUM_CHUNKS = 256 // CHUNK
NUM_ACC = 16
SIN = (3.14159265353629, -5.16771276462444, 2.550163318944362, -0.5992521977957433, 0.08205040168394097, -0.00702838621010907)
COS = (0.9999999997799045, -4.9348021370788056, 4.058709159555753, -1.3352120030448535, 0.23493731379172217, -0.024396324310603436)
MESH = pl.DeviceIdType.MESH
PARTS = tuple(pl.ds(n * 64, 64) for n in range(8))
HOMES = ((1, 0), (2, 2))


def sincos_turns(u):
    magic = 12582912.0
    f = u - ((u + magic) - magic)
    z = f * f
    sin_h = f * (SIN[0] + z * (SIN[1] + z * (SIN[2] + z * (SIN[3] + z * (SIN[4] + z * SIN[5])))))
    cos_h = COS[0] + z * (COS[1] + z * (COS[2] + z * (COS[3] + z * (COS[4] + z * COS[5]))))
    twice = sin_h + sin_h
    return twice * cos_h, 1.0 - twice * sin_h


def split3(x):
    a = x.astype(BF16)
    r = x - a.astype(F32)
    b = r.astype(BF16)
    c = (r - b.astype(F32)).astype(BF16)
    return a, b, c


def butterfly8(v):
    for step in (4, 2, 1):
        out = list(v)
        for i in range(8):
            if not i & step:
                out[i] = v[i] + v[i + step]
                out[i + step] = v[i] - v[i + step]
        v = out
    return v


def popcount_tile(shape):
    sub = lax.broadcasted_iota(jnp.int32, shape, 0)
    lane = lax.broadcasted_iota(jnp.int32, shape, 1)
    total = jnp.zeros(shape, jnp.int32)
    for b in range(3):
        total = total + ((sub >> b) & 1)
    for b in range(7):
        total = total + ((lane >> b) & 1)
    return total.astype(F32)


def fold(x):
    return jnp.sum(x.reshape(-1, 8, 128), axis=0)


def cols_of(ct):
    return pl.ds(ct * 128, 128)


def rotate(values, cos_b, sin_b):
    kr, ki, orr, oi = values
    return (cos_b * kr + sin_b * oi, cos_b * ki - sin_b * orr, cos_b * orr + sin_b * ki, cos_b * oi - sin_b * kr)


def groups(i):
    for g in range(CHUNK // 16):
        for ct in range(2):
            start = pl.multiple_of(i * CHUNK + g * 16, 16)
            cost_start = pl.multiple_of(ct * 256 + i * CHUNK + g * 16, 16)
            yield pl.ds(g * 16, 16), pl.ds(start, 16), cols_of(ct), pl.ds(cost_start, 16)


def loop(count, body):
    def step(n, carry):
        body(n)
        return carry
    lax.fori_loop(0, count, step, 0)


def kernel(cost, gamma, beta, had, out, stash, keep, other, cc, tab, saved, hat, diag, rot, acc,
           wide, flip, big, mine, res, c_send, c_recv, f_send, f_recv, x_send, x_recv, h_out, h_in, r_send, r_recv, relay_send, relay_recv, credit):
    inst = lax.axis_index('inst')
    qy = lax.axis_index('qy')
    qx = lax.axis_index('qx')
    core = lax.rem(qx, 2)
    my_set = qx // 2
    active = qy == my_set + 1
    partner = (inst, qy, qx + 1 - 2 * core)
    kind = lax.rem(qy // 2 + qy, 2)

    barrier = pltpu.get_barrier_semaphore()
    for a in range(4):
        for b in range(4):
            @pl.when((qy != a) | (qx != b))
            def _():
                pl.semaphore_signal(barrier, inc=1, device_id=(inst, a, b), device_id_type=MESH)
    pl.semaphore_wait(barrier, 15)

    def view(s):
        return (qy, qx, qx // 2) if s == 0 else (3 - qy, qx, 1 - qx // 2)

    def home_copy(s, src, origin_y, origin_x, send_sem, part=None):
        home_y, home_x = HOMES[s]
        slot = lax.rem(origin_y // 2 + origin_y, 2)
        dst = cc.at[slot, origin_x]
        if part is not None:
            src, dst = src.at[part], dst.at[part]
        return pltpu.make_async_remote_copy(
            src_ref=src, dst_ref=dst, send_sem=send_sem, recv_sem=c_recv.at[slot, origin_x],
            device_id=(inst, home_y, home_x + origin_y // 2), device_id_type=MESH)

    def relay_copies(s, to_y, to_x, r):
        return [pltpu.make_async_remote_copy(
            src_ref=cost.at[part], dst_ref=cc.at[2, r].at[part], send_sem=c_send.at[s], recv_sem=relay_recv.at[r, n],
            device_id=(inst, to_y, to_x), device_id_type=MESH) for n, part in enumerate(PARTS)]

    def is_self(s):
        home_y, home_x = HOMES[s]
        return (qy == home_y) & (qx == home_x + qy // 2)

    def routes(s):
        y, _x, side = view(s)
        near_y = 1 if s == 0 else 2
        corner_y = 0 if s == 0 else 3
        corner_x = qx - 2 if s == 0 else qx + 2
        direct = jnp.logical_not(is_self(s)) & ((side == 0) | (y == 1))
        return [(direct, [home_copy(s, cost, qy, qx, c_send.at[s])]),
                ((side == 1) & (y == 0), relay_copies(s, corner_y, corner_x, 0)),
                ((side == 1) & (y == 2), relay_copies(s, near_y, qx, 0)),
                ((side == 1) & (y == 3), relay_copies(s, near_y, qx, 1))]

    def relays(s):
        y, _x, side = view(s)
        corner_y = 0 if s == 0 else 3
        corner_x = qx + 2 if s == 0 else qx - 2
        far = (2, 3) if s == 0 else (1, 0)
        return [((side == 0) & (y == 0), [(0, corner_y, corner_x)]),
                ((side == 1) & (y == 1), [(r, far[r], qx) for r in range(2)])]

    for s in range(2):
        @pl.when(is_self(s))
        def _():
            pltpu.make_async_copy(cost, cc.at[kind, qx], c_recv.at[kind, qx]).start()

        for condition, copies in routes(s):
            @pl.when(condition)
            def _():
                for copy in copies:
                    copy.start()

    for s in range(2):
        for condition, blocks in relays(s):
            @pl.when(condition)
            def _():
                for n, part in enumerate(PARTS):
                    for r, origin_y, origin_x in blocks:
                        pltpu.make_async_copy(cost.at[part], cc.at[2, r].at[part], relay_recv.at[r, n]).wait()
                        home_copy(s, cc.at[2, r], origin_y, origin_x, relay_send.at[r], part).start()

    def cost_arrived(which, j):
        pltpu.make_async_copy(cost, cc.at[which, j], c_recv.at[which, j]).wait()

    def forward_copy(j):
        return pltpu.make_async_remote_copy(
            src_ref=cc.at[1, j], dst_ref=cc.at[2, j], send_sem=f_send.at[j], recv_sem=f_recv.at[j],
            device_id=partner, device_id_type=MESH)

    def exchange(parity, i):
        rows = pl.ds(pl.multiple_of(i * CHUNK, CHUNK), CHUNK)
        return pltpu.make_async_remote_copy(
            src_ref=other.at[1 - parity, :, :, rows, :], dst_ref=other.at[parity, :, :, rows, :],
            send_sem=x_send.at[parity, i], recv_sem=x_recv.at[parity, i],
            device_id=partner, device_id_type=MESH)

    def release(i):
        pl.semaphore_signal(credit.at[i], inc=1, device_id=partner, device_id_type=MESH)

    def send(parity, i, first=None):
        if first is None:
            pl.semaphore_wait(credit.at[i], 1)
        else:
            @pl.when(jnp.logical_not(first))
            def _():
                pl.semaphore_wait(credit.at[i], 1)
        exchange(parity, i).start()

    def stash_out(n):
        return pltpu.make_async_copy(hat.at[lax.rem(n, 2)], stash.at[n], h_out.at[lax.rem(n, 2)])

    def stash_in(n):
        return pltpu.make_async_copy(stash.at[n], hat.at[lax.rem(n, 2)], h_in.at[lax.rem(n, 2)])

    def multiply(strips):
        h = had[...]
        for read, write in strips:
            parts = jnp.dot(jnp.concatenate(split3(read()), axis=0), h, preferred_element_type=F32)
            write(parts[0:STRIP] + parts[STRIP:2 * STRIP] + parts[2 * STRIP:3 * STRIP])

    def state_tile(par, t, rows):
        comp, half, j = t // 8, (t // 4) % 2, t % 4
        return keep.at[comp, j, rows, :] if half == 0 else other.at[par, comp, j, rows, :]

    def pair(src, dst):
        def read():
            return src[...]

        def write(value):
            dst[...] = value
        return read, write

    def to_state(par, i):
        rows = pl.ds(pl.multiple_of(i * CHUNK, CHUNK), CHUNK)
        multiply([pair(big.at[t], state_tile(par, t, rows)) for t in range(16)])

    def from_state(par, i):
        rows = pl.ds(pl.multiple_of(i * CHUNK, CHUNK), CHUNK)
        multiply([pair(state_tile(par, t, rows), big.at[t]) for t in range(16)])

    def load_state(par, rows, cols, j):
        return (keep[0, j, rows, cols], keep[1, j, rows, cols],
                other[par, 0, j, rows, cols], other[par, 1, j, rows, cols])

    def store_state(par, rows, cols, j, values):
        keep[0, j, rows, cols] = values[0]
        keep[1, j, rows, cols] = values[1]
        other[par, 0, j, rows, cols] = values[2]
        other[par, 1, j, rows, cols] = values[3]

    def spread(re, im, local_rows, cols):
        for comp, v in enumerate((butterfly8(re), butterfly8(im))):
            for t in range(8):
                big[comp * 8 + t, local_rows, cols] = v[t]

    def gather_big(local_rows, cols):
        re = butterfly8([big[t, local_rows, cols] for t in range(8)])
        im = butterfly8([big[8 + t, local_rows, cols] for t in range(8)])
        return re, im

    def middle(layer, par, forward):
        slot = lax.rem(layer, 2)

        def first(j, half):
            for comp in range(2):
                src = keep[comp, j] if half == 0 else other[par, comp, j]
                flip[half * 2 + comp] = src.T
            multiply([pair(flip.at[half * 2 + comp, pl.ds(r * STRIP, STRIP), :], wide.at[half * 2 + comp, pl.ds(r * STRIP, STRIP), :])
                      for comp in range(2) for r in range(256 // STRIP)])

        def second(j, total, half):
            n = half * 4 + j
            bits = half + j // 2 + lax.rem(j, 2)
            for g in range(16):
                rows = pl.ds(g * 16, 16)
                for ct in range(2):
                    cols = cols_of(ct)
                    q0 = bin(2 * g).count('1') + ct
                    q1 = bin(2 * g + 1).count('1') + ct

                    def pick(m):
                        return jnp.concatenate([diag[layer, m, bits + q0], diag[layer, m, bits + q1]], axis=0)
                    re, im = wide[half * 2, rows, cols], wide[half * 2 + 1, rows, cols]
                    dc, ds = pick(0), pick(1)
                    if forward:
                        re, im = re * dc + im * ds, im * dc - re * ds
                        hat[slot, 0, n, rows, cols] = re
                        hat[slot, 1, n, rows, cols] = im
                    else:
                        term = re * hat[slot, 1, n, rows, cols] - im * hat[slot, 0, n, rows, cols]
                        total = total + fold(term * pick(2))
                        re, im = re * dc - im * ds, im * dc + re * ds
                    wide[half * 2, rows, cols] = re
                    wide[half * 2 + 1, rows, cols] = im
            multiply([pair(wide.at[half * 2 + comp, pl.ds(r * STRIP, STRIP), :], flip.at[half * 2 + comp, pl.ds(r * STRIP, STRIP), :])
                      for comp in range(2) for r in range(256 // STRIP)])
            for comp in range(2):
                value = flip[half * 2 + comp].T
                if half == 0:
                    keep[comp, j] = value
                else:
                    other[par, comp, j] = value
            return total

        def body(j, total):
            first(j, 0)
            first(j, 1)
            return second(j, second(j, total, 0), 1)
        return lax.fori_loop(0, 4, body, jnp.zeros((8, 128), F32))

    def tables():
        pop = popcount_tile((8, 128))
        for layer in range(LAYERS):
            half_angle = jnp.full((8, 128), 0.25 / math.pi, F32) * beta[my_set, layer]

            def entry(q):
                weight = (LOCAL_QUBITS - 2 * q).astype(F32) - 2.0 * pop
                sin_d, cos_d = sincos_turns(half_angle * weight)
                diag[layer, 0, q] = cos_d * (2.0 ** -LOCAL_QUBITS)
                diag[layer, 1, q] = sin_d * (2.0 ** -LOCAL_QUBITS)
                diag[layer, 2, q] = weight
            loop(10, entry)
            sin_h, cos_h = sincos_turns(jnp.concatenate([half_angle, half_angle], axis=0))
            rot[layer + 1, 0] = cos_h
            rot[layer + 1, 1] = sin_h
        rot[0, 0] = jnp.ones((16, 128), F32)
        rot[0, 1] = jnp.zeros((16, 128), F32)
        acc[...] = jnp.zeros((NUM_ACC, 8, 128), F32)

        def init(r):
            rows = pl.ds(pl.multiple_of(r * 16, 16), 16)
            for j in range(4):
                start = jnp.full((16, 256), 2.0 ** -10, F32)
                zero = jnp.zeros((16, 256), F32)
                keep[0, j, rows, :] = start
                keep[1, j, rows, :] = zero
                other[0, 0, j, rows, :] = start
                other[0, 1, j, rows, :] = zero
        loop(16, init)

    def fill(layer, which, half, j):
        turns = gamma[my_set, layer] * (0.5 / math.pi)

        def rows_body(r):
            start = pl.multiple_of(r * 32, 32)
            for ct in range(2):
                cost_rows = pl.ds(pl.multiple_of(ct * 256 + start, 32), 32)
                sin_p, cos_p = sincos_turns(turns * cc[which, j, cost_rows, :])
                tab[layer, 0, half * 4 + j, pl.ds(start, 32), cols_of(ct)] = cos_p
                tab[layer, 1, half * 4 + j, pl.ds(start, 32), cols_of(ct)] = sin_p
        loop(8, rows_body)

    def arrive():
        def own(j):
            cost_arrived(1, j)
            forward_copy(j).start()
            loop(3, lambda n: fill(2 * n, 1, 1, j))

        def passed(j):
            forward_copy(j).wait()
            loop(2, lambda n: fill(2 * n + 1, 2, 1, j))

        def kept(j):
            cost_arrived(0, j)
            loop(LAYERS, lambda n: fill(n, 0, 0, j))
        def near_then_far(step):
            near = lax.rem(step + my_set, 2) * 2
            loop(2, lambda n: own(near + n))

            @pl.when(step == 1)
            def _():
                loop(4, passed)
            loop(2, lambda n: kept(near + n))
        loop(2, near_then_far)

    def forward_layer(layer):
        par = lax.rem(layer, 2)

        def alpha(i):
            @pl.when(layer > 0)
            def _():
                exchange(par, i).wait()
                release(i)
            cos_b, sin_b = rot[layer, 0], rot[layer, 1]
            for local_rows, rows, cols, _c in groups(i):
                re, im = [None] * 8, [None] * 8
                for j in range(4):
                    v = rotate(load_state(par, rows, cols, j), cos_b, sin_b)
                    for half in range(2):
                        n = half * 4 + j
                        pr, pi = v[2 * half], v[2 * half + 1]
                        saved[layer, 0, n, rows, cols] = pr
                        saved[layer, 1, n, rows, cols] = pi
                        c, s = tab[layer, 0, n, rows, cols], tab[layer, 1, n, rows, cols]
                        re[n], im[n] = pr * c + pi * s, pi * c - pr * s
                spread(re, im, local_rows, cols)
            to_state(par, i)
        loop(NUM_CHUNKS, alpha)

        @pl.when((layer >= 2))
        def _():
            stash_out(layer - 2).wait()
        middle(layer, par, True)

        @pl.when(layer < 3)
        def _():
            stash_out(layer).start()

        def gamma_sweep(i):
            from_state(par, i)
            for local_rows, rows, cols, _c in groups(i):
                re, im = gather_big(local_rows, cols)
                for j in range(4):
                    store_state(par, rows, cols, j, (re[j], im[j], re[4 + j], im[4 + j]))

            send(1 - par, i, layer == 0)
        loop(NUM_CHUNKS, gamma_sweep)

    def final(i):
        exchange(1, i).wait()
        release(i)
        energy = jnp.zeros((8, 128), F32)
        grad = jnp.zeros((8, 128), F32)
        cos_b, sin_b = rot[LAYERS, 0], rot[LAYERS, 1]
        for local_rows, rows, cols, crows in groups(i):
            for j in range(4):
                kr, ki, orr, oi = rotate(load_state(1, rows, cols, j), cos_b, sin_b)
                ck, co = cc[0, j, crows, :], cc[2, j, crows, :]
                lam = (ck * kr, ck * ki, co * orr, co * oi)
                energy = energy + fold(lam[0] * kr + lam[1] * ki + lam[2] * orr + lam[3] * oi)
                grad = grad + fold((ck - co) * (kr * oi - ki * orr))
                store_state(1, rows, cols, j, rotate(lam, cos_b, -sin_b))
        acc[0] = acc[0] + energy
        acc[2 * LAYERS] = acc[2 * LAYERS] + grad

        send(0, i)

    def backward_layer(step):
        layer = LAYERS - 1 - step
        par = lax.rem(layer, 2)

        def alpha(i):
            exchange(par, i).wait()

            @pl.when(layer > 0)
            def _():
                release(i)
            for local_rows, rows, cols, _c in groups(i):
                v = [load_state(par, rows, cols, j) for j in range(4)]
                re = [v[j][0] for j in range(4)] + [v[j][2] for j in range(4)]
                im = [v[j][1] for j in range(4)] + [v[j][3] for j in range(4)]
                spread(re, im, local_rows, cols)
            to_state(par, i)
        loop(NUM_CHUNKS, alpha)

        @pl.when(layer < 3)
        def _():
            stash_in(layer).wait()
        total = middle(layer, par, False)
        acc[LAYERS + 1 + layer] = acc[LAYERS + 1 + layer] + total

        @pl.when(layer >= 2)
        def _():
            stash_in(layer - 2).start()

        def gamma_sweep(i):
            from_state(par, i)
            g_sum = jnp.zeros((8, 128), F32)
            b_sum = jnp.zeros((8, 128), F32)
            cos_b, sin_b = rot[layer, 0], rot[layer, 1]
            for local_rows, rows, cols, crows in groups(i):
                re, im = gather_big(local_rows, cols)
                for j in range(4):
                    lam, psi = [], []
                    for half in range(2):
                        n = half * 4 + j
                        c, s = tab[layer, 0, n, rows, cols], tab[layer, 1, n, rows, cols]
                        lr, li = re[n] * c - im[n] * s, im[n] * c + re[n] * s
                        pr, pi = saved[layer, 0, n, rows, cols], saved[layer, 1, n, rows, cols]
                        cost_n = cc[0, j, crows, :] if half == 0 else cc[1 + par, j, crows, :]
                        g_sum = g_sum + fold(cost_n * (lr * pi - li * pr))
                        lam += [lr, li]
                        psi += [pr, pi]
                    b_sum = b_sum + fold(lam[0] * psi[3] - lam[1] * psi[2] + lam[2] * psi[1] - lam[3] * psi[0])
                    store_state(par, rows, cols, j, rotate(lam, cos_b, -sin_b))
            acc[1 + layer] = acc[1 + layer] + 2.0 * g_sum

            @pl.when(layer > 0)
            def _():
                acc[LAYERS + layer] = acc[LAYERS + layer] + b_sum

            @pl.when(layer > 0)
            def _():
                send(1 - par, i)
        loop(NUM_CHUNKS, gamma_sweep)

    def result_copy(a, b):
        return pltpu.make_async_remote_copy(
            src_ref=mine.at[0:NUM_ACC], dst_ref=res.at[qx], send_sem=r_send.at[a * 4 + b], recv_sem=r_recv.at[qx],
            device_id=(inst, a, b), device_id_type=MESH)

    def others(fn):
        for a in range(4):
            for b in range(4):
                @pl.when((qy != a) | (qx != b))
                def _():
                    fn(result_copy(a, b))

    @pl.when(active)
    def _():
        tables()
        arrive()
        loop(LAYERS, forward_layer)
        loop(NUM_CHUNKS, final)
        loop(LAYERS, backward_layer)
        mine[0:NUM_ACC] = jnp.sum(acc[...], axis=1)
        res[qx] = mine[0:NUM_ACC]
        others(lambda copy: copy.start())

    for slot in range(4):
        @pl.when(jnp.logical_not(active & (qx == slot)))
        def _():
            pltpu.make_async_remote_copy(
                src_ref=mine.at[0:NUM_ACC], dst_ref=res.at[slot], send_sem=r_send.at[0], recv_sem=r_recv.at[slot],
                device_id=partner, device_id_type=MESH).wait_recv()

    for s in range(2):
        total = jnp.sum(res[2 * s] + res[2 * s + 1], axis=1, keepdims=True)
        out[s] = jnp.broadcast_to(total, (NUM_ACC, 128))

    for s in range(2):
        @pl.when(jnp.logical_not(is_self(s)))
        def _():
            home_copy(s, cost, qy, qx, c_send.at[s]).wait_send()

        for condition, blocks in relays(s):
            @pl.when(condition)
            def _():
                for r, origin_y, origin_x in blocks:
                    home_copy(s, cc.at[2, r], origin_y, origin_x, relay_send.at[r]).wait_send()

    @pl.when(active)
    def _():
        others(lambda copy: copy.wait_send())


def hadamard():
    index = np.arange(256)
    both = index[:, None] & index[None, :]
    parity = sum((both >> b) & 1 for b in range(8)) & 1
    return jnp.asarray(1.0 - 2.0 * parity, BF16)


def solution(mesh):
    def device_fn(cost, gamma, beta):
        vmem = pltpu.VMEM
        dma = pltpu.SemaphoreType.DMA
        tile = (256, 256)
        out, _ = pl.pallas_call(
            kernel,
            out_shape=(jax.ShapeDtypeStruct((2, NUM_ACC, 128), F32), jax.ShapeDtypeStruct((3, 2, 8) + tile, F32)),
            in_specs=[pl.BlockSpec(memory_space=pl.ANY), pl.BlockSpec(memory_space=pltpu.SMEM),
                      pl.BlockSpec(memory_space=pltpu.SMEM), pl.BlockSpec(memory_space=pltpu.VMEM)],
            out_specs=(pl.BlockSpec(memory_space=pltpu.VMEM), pl.BlockSpec(memory_space=pl.ANY)),
            scratch_shapes=[
                vmem((2, 4) + tile, F32),
                vmem((2, 2, 4) + tile, F32),
                vmem((3, 4, 512, 128), F32),
                vmem((LAYERS, 2, 8) + tile, F32),
                vmem((LAYERS, 2, 8) + tile, F32),
                vmem((2, 2, 8) + tile, F32),
                vmem((LAYERS, 3, 12, 8, 128), F32),
                vmem((LAYERS + 1, 2, 16, 128), F32),
                vmem((NUM_ACC, 8, 128), F32),
                vmem((4,) + tile, F32),
                vmem((4,) + tile, F32),
                vmem((16, CHUNK, 256), F32),
                vmem((2 * NUM_ACC, 128), F32),
                vmem((4, NUM_ACC, 128), F32),
                dma((2,)), dma((2, 4)), dma((4,)), dma((4,)), dma((2, NUM_CHUNKS)), dma((2, NUM_CHUNKS)),
                dma((2,)), dma((2,)), dma((16,)), dma((4,)), dma((2,)), dma((2, len(PARTS))), pltpu.SemaphoreType.REGULAR((NUM_CHUNKS,)),
            ],
            compiler_params=pltpu.CompilerParams(collective_id=0, has_side_effects=True, vmem_limit_bytes=67043328),
        )(cost.reshape(512, 128), gamma, beta, hadamard())
        return out[:, 0, 0], out[:, 1:1 + 2 * LAYERS, 0]

    cost_spec = P(('inst', 'qy', 'qx'))
    angle_spec = P('inst', None)
    return jax.shard_map(device_fn, mesh=mesh, in_specs=(cost_spec, angle_spec, angle_spec), out_specs=(P('inst'), angle_spec), check_vma=False)
```

```python
import math
import numpy as np
import jax
import jax.numpy as jnp
from jax import lax
from jax.experimental import pallas as pl
from jax.experimental.pallas import tpu as pltpu
from jax.sharding import PartitionSpec as P

F32 = jnp.float32
BF16 = jnp.bfloat16
LAYERS = 5
LOCAL_QUBITS = 19
CHUNK = 64
STRIP = 64
NUM_CHUNKS = 256 // CHUNK
NUM_ACC = 16
SIN = (3.14159265353629, -5.16771276462444, 2.550163318944362, -0.5992521977957433, 0.08205040168394097, -0.00702838621010907)
COS = (0.9999999997799045, -4.9348021370788056, 4.058709159555753, -1.3352120030448535, 0.23493731379172217, -0.024396324310603436)
MESH = pl.DeviceIdType.MESH
PARTS = tuple(pl.ds(n * 128, 128) for n in range(4))
HOMES = ((1, 0), (2, 2))


def sincos_turns(u):
    magic = 12582912.0
    f = u - ((u + magic) - magic)
    z = f * f
    sin_h = f * (SIN[0] + z * (SIN[1] + z * (SIN[2] + z * (SIN[3] + z * (SIN[4] + z * SIN[5])))))
    cos_h = COS[0] + z * (COS[1] + z * (COS[2] + z * (COS[3] + z * (COS[4] + z * COS[5]))))
    twice = sin_h + sin_h
    return twice * cos_h, 1.0 - twice * sin_h


def split3(x):
    a = x.astype(BF16)
    r = x - a.astype(F32)
    b = r.astype(BF16)
    c = (r - b.astype(F32)).astype(BF16)
    return a, b, c


def butterfly8(v):
    for step in (4, 2, 1):
        out = list(v)
        for i in range(8):
            if not i & step:
                out[i] = v[i] + v[i + step]
                out[i + step] = v[i] - v[i + step]
        v = out
    return v


def popcount_tile(shape):
    sub = lax.broadcasted_iota(jnp.int32, shape, 0)
    lane = lax.broadcasted_iota(jnp.int32, shape, 1)
    total = jnp.zeros(shape, jnp.int32)
    for b in range(3):
        total = total + ((sub >> b) & 1)
    for b in range(7):
        total = total + ((lane >> b) & 1)
    return total.astype(F32)


def fold(x):
    return jnp.sum(x.reshape(-1, 8, 128), axis=0)


def cols_of(ct):
    return pl.ds(ct * 128, 128)


def rotate(values, cos_b, sin_b):
    kr, ki, orr, oi = values
    return (cos_b * kr + sin_b * oi, cos_b * ki - sin_b * orr, cos_b * orr + sin_b * ki, cos_b * oi - sin_b * kr)


def groups(i):
    for g in range(CHUNK // 16):
        for ct in range(2):
            start = pl.multiple_of(i * CHUNK + g * 16, 16)
            cost_start = pl.multiple_of(ct * 256 + i * CHUNK + g * 16, 16)
            yield pl.ds(g * 16, 16), pl.ds(start, 16), cols_of(ct), pl.ds(cost_start, 16)


def loop(count, body):
    def step(n, carry):
        body(n)
        return carry
    lax.fori_loop(0, count, step, 0)


def kernel(cost, gamma, beta, had, out, stash, keep, other, cc, tab, saved, hat, diag, rot, acc,
           wide, flip, big, mine, res, c_send, c_recv, f_send, f_recv, x_send, x_recv, h_out, h_in, r_send, r_recv, relay_send, relay_recv, credit):
    inst = lax.axis_index('inst')
    qy = lax.axis_index('qy')
    qx = lax.axis_index('qx')
    core = lax.rem(qx, 2)
    my_set = qx // 2
    active = qy == my_set + 1
    partner = (inst, qy, qx + 1 - 2 * core)
    kind = lax.rem(qy // 2 + qy, 2)

    barrier = pltpu.get_barrier_semaphore()
    for a in range(4):
        for b in range(4):
            @pl.when((qy != a) | (qx != b))
            def _():
                pl.semaphore_signal(barrier, inc=1, device_id=(inst, a, b), device_id_type=MESH)
    pl.semaphore_wait(barrier, 15)

    def view(s):
        return (qy, qx, qx // 2) if s == 0 else (3 - qy, qx, 1 - qx // 2)

    def home_copy(s, src, origin_y, origin_x, send_sem, part=None):
        home_y, home_x = HOMES[s]
        slot = lax.rem(origin_y // 2 + origin_y, 2)
        dst = cc.at[slot, origin_x]
        if part is not None:
            src, dst = src.at[part], dst.at[part]
        return pltpu.make_async_remote_copy(
            src_ref=src, dst_ref=dst, send_sem=send_sem, recv_sem=c_recv.at[slot, origin_x],
            device_id=(inst, home_y, home_x + origin_y // 2), device_id_type=MESH)

    def relay_copies(s, to_y, to_x, r):
        return [pltpu.make_async_remote_copy(
            src_ref=cost.at[part], dst_ref=cc.at[2, r].at[part], send_sem=c_send.at[s], recv_sem=relay_recv.at[r, n],
            device_id=(inst, to_y, to_x), device_id_type=MESH) for n, part in enumerate(PARTS)]

    def is_self(s):
        home_y, home_x = HOMES[s]
        return (qy == home_y) & (qx == home_x + qy // 2)

    def routes(s):
        y, _x, side = view(s)
        near_y = 1 if s == 0 else 2
        corner_y = 0 if s == 0 else 3
        corner_x = qx - 2 if s == 0 else qx + 2
        direct = jnp.logical_not(is_self(s)) & ((side == 0) | (y == 1))
        return [(direct, [home_copy(s, cost, qy, qx, c_send.at[s])]),
                ((side == 1) & (y == 0), relay_copies(s, corner_y, corner_x, 0)),
                ((side == 1) & (y == 2), relay_copies(s, near_y, qx, 0)),
                ((side == 1) & (y == 3), relay_copies(s, near_y, qx, 1))]

    def relays(s):
        y, _x, side = view(s)
        corner_y = 0 if s == 0 else 3
        corner_x = qx + 2 if s == 0 else qx - 2
        far = (2, 3) if s == 0 else (1, 0)
        return [((side == 0) & (y == 0), [(0, corner_y, corner_x)]),
                ((side == 1) & (y == 1), [(r, far[r], qx) for r in range(2)])]

    for s in range(2):
        @pl.when(is_self(s))
        def _():
            pltpu.make_async_copy(cost, cc.at[kind, qx], c_recv.at[kind, qx]).start()

        for condition, copies in routes(s):
            @pl.when(condition)
            def _():
                for copy in copies:
                    copy.start()

    for s in range(2):
        for condition, blocks in relays(s):
            @pl.when(condition)
            def _():
                for n, part in enumerate(PARTS):
                    for r, origin_y, origin_x in blocks:
                        pltpu.make_async_copy(cost.at[part], cc.at[2, r].at[part], relay_recv.at[r, n]).wait()
                        home_copy(s, cc.at[2, r], origin_y, origin_x, relay_send.at[r], part).start()

    def cost_arrived(which, j):
        pltpu.make_async_copy(cost, cc.at[which, j], c_recv.at[which, j]).wait()

    def forward_copy(j):
        return pltpu.make_async_remote_copy(
            src_ref=cc.at[1, j], dst_ref=cc.at[2, j], send_sem=f_send.at[j], recv_sem=f_recv.at[j],
            device_id=partner, device_id_type=MESH)

    def exchange(parity, i):
        rows = pl.ds(pl.multiple_of(i * CHUNK, CHUNK), CHUNK)
        return pltpu.make_async_remote_copy(
            src_ref=other.at[1 - parity, :, :, rows, :], dst_ref=other.at[parity, :, :, rows, :],
            send_sem=x_send.at[parity, i], recv_sem=x_recv.at[parity, i],
            device_id=partner, device_id_type=MESH)

    def release(i):
        pl.semaphore_signal(credit.at[i], inc=1, device_id=partner, device_id_type=MESH)

    def send(parity, i, first=None):
        if first is None:
            pl.semaphore_wait(credit.at[i], 1)
        else:
            @pl.when(jnp.logical_not(first))
            def _():
                pl.semaphore_wait(credit.at[i], 1)
        exchange(parity, i).start()

    def stash_out(n):
        return pltpu.make_async_copy(hat.at[lax.rem(n, 2)], stash.at[n], h_out.at[lax.rem(n, 2)])

    def stash_in(n):
        return pltpu.make_async_copy(stash.at[n], hat.at[lax.rem(n, 2)], h_in.at[lax.rem(n, 2)])

    def multiply(strips):
        h = had[...]
        for read, write in strips:
            parts = jnp.dot(jnp.concatenate(split3(read()), axis=0), h, preferred_element_type=F32)
            write(parts[0:STRIP] + parts[STRIP:2 * STRIP] + parts[2 * STRIP:3 * STRIP])

    def state_tile(par, t, rows):
        comp, half, j = t // 8, (t // 4) % 2, t % 4
        return keep.at[comp, j, rows, :] if half == 0 else other.at[par, comp, j, rows, :]

    def pair(src, dst):
        def read():
            return src[...]

        def write(value):
            dst[...] = value
        return read, write

    def to_state(par, i):
        rows = pl.ds(pl.multiple_of(i * CHUNK, CHUNK), CHUNK)
        multiply([pair(big.at[t], state_tile(par, t, rows)) for t in range(16)])

    def from_state(par, i):
        rows = pl.ds(pl.multiple_of(i * CHUNK, CHUNK), CHUNK)
        multiply([pair(state_tile(par, t, rows), big.at[t]) for t in range(16)])

    def load_state(par, rows, cols, j):
        return (keep[0, j, rows, cols], keep[1, j, rows, cols],
                other[par, 0, j, rows, cols], other[par, 1, j, rows, cols])

    def store_state(par, rows, cols, j, values):
        keep[0, j, rows, cols] = values[0]
        keep[1, j, rows, cols] = values[1]
        other[par, 0, j, rows, cols] = values[2]
        other[par, 1, j, rows, cols] = values[3]

    def spread(re, im, local_rows, cols):
        for comp, v in enumerate((butterfly8(re), butterfly8(im))):
            for t in range(8):
                big[comp * 8 + t, local_rows, cols] = v[t]

    def gather_big(local_rows, cols):
        re = butterfly8([big[t, local_rows, cols] for t in range(8)])
        im = butterfly8([big[8 + t, local_rows, cols] for t in range(8)])
        return re, im

    def middle(layer, par, forward):
        slot = lax.rem(layer, 2)

        def first(j, half):
            for comp in range(2):
                src = keep[comp, j] if half == 0 else other[par, comp, j]
                flip[half * 2 + comp] = src.T
            multiply([pair(flip.at[half * 2 + comp, pl.ds(r * STRIP, STRIP), :], wide.at[half * 2 + comp, pl.ds(r * STRIP, STRIP), :])
                      for comp in range(2) for r in range(256 // STRIP)])

        def second(j, total, half):
            n = half * 4 + j
            bits = half + j // 2 + lax.rem(j, 2)
            for g in range(16):
                rows = pl.ds(g * 16, 16)
                for ct in range(2):
                    cols = cols_of(ct)
                    q0 = bin(2 * g).count('1') + ct
                    q1 = bin(2 * g + 1).count('1') + ct

                    def pick(m):
                        return jnp.concatenate([diag[layer, m, bits + q0], diag[layer, m, bits + q1]], axis=0)
                    re, im = wide[half * 2, rows, cols], wide[half * 2 + 1, rows, cols]
                    dc, ds = pick(0), pick(1)
                    if forward:
                        re, im = re * dc + im * ds, im * dc - re * ds
                        hat[slot, 0, n, rows, cols] = re
                        hat[slot, 1, n, rows, cols] = im
                    else:
                        term = re * hat[slot, 1, n, rows, cols] - im * hat[slot, 0, n, rows, cols]
                        total = total + fold(term * pick(2))
                        re, im = re * dc - im * ds, im * dc + re * ds
                    wide[half * 2, rows, cols] = re
                    wide[half * 2 + 1, rows, cols] = im
            multiply([pair(wide.at[half * 2 + comp, pl.ds(r * STRIP, STRIP), :], flip.at[half * 2 + comp, pl.ds(r * STRIP, STRIP), :])
                      for comp in range(2) for r in range(256 // STRIP)])
            for comp in range(2):
                value = flip[half * 2 + comp].T
                if half == 0:
                    keep[comp, j] = value
                else:
                    other[par, comp, j] = value
            return total

        def body(j, total):
            first(j, 0)
            first(j, 1)
            return second(j, second(j, total, 0), 1)
        return lax.fori_loop(0, 4, body, jnp.zeros((8, 128), F32))

    def tables():
        pop = popcount_tile((8, 128))
        for layer in range(LAYERS):
            half_angle = jnp.full((8, 128), 0.25 / math.pi, F32) * beta[my_set, layer]

            def entry(q):
                weight = (LOCAL_QUBITS - 2 * q).astype(F32) - 2.0 * pop
                sin_d, cos_d = sincos_turns(half_angle * weight)
                diag[layer, 0, q] = cos_d * (2.0 ** -LOCAL_QUBITS)
                diag[layer, 1, q] = sin_d * (2.0 ** -LOCAL_QUBITS)
                diag[layer, 2, q] = weight
            loop(10, entry)
            sin_h, cos_h = sincos_turns(jnp.concatenate([half_angle, half_angle], axis=0))
            rot[layer + 1, 0] = cos_h
            rot[layer + 1, 1] = sin_h
        rot[0, 0] = jnp.ones((16, 128), F32)
        rot[0, 1] = jnp.zeros((16, 128), F32)
        acc[...] = jnp.zeros((NUM_ACC, 8, 128), F32)

        def init(r):
            rows = pl.ds(pl.multiple_of(r * 16, 16), 16)
            for j in range(4):
                start = jnp.full((16, 256), 2.0 ** -10, F32)
                zero = jnp.zeros((16, 256), F32)
                keep[0, j, rows, :] = start
                keep[1, j, rows, :] = zero
                other[0, 0, j, rows, :] = start
                other[0, 1, j, rows, :] = zero
        loop(16, init)

    def fill(layer, which, half, j):
        turns = gamma[my_set, layer] * (0.5 / math.pi)

        def rows_body(r):
            start = pl.multiple_of(r * 32, 32)
            for ct in range(2):
                cost_rows = pl.ds(pl.multiple_of(ct * 256 + start, 32), 32)
                sin_p, cos_p = sincos_turns(turns * cc[which, j, cost_rows, :])
                tab[layer, 0, half * 4 + j, pl.ds(start, 32), cols_of(ct)] = cos_p
                tab[layer, 1, half * 4 + j, pl.ds(start, 32), cols_of(ct)] = sin_p
        loop(8, rows_body)

    def arrive():
        def own(j):
            cost_arrived(1, j)
            forward_copy(j).start()
            loop(3, lambda n: fill(2 * n, 1, 1, j))

        def passed(j):
            forward_copy(j).wait()
            loop(2, lambda n: fill(2 * n + 1, 2, 1, j))

        def kept(j):
            cost_arrived(0, j)
            loop(LAYERS, lambda n: fill(n, 0, 0, j))
        def near_then_far(step):
            near = lax.rem(step + my_set, 2) * 2
            loop(2, lambda n: own(near + n))
            loop(2, lambda n: passed(near + n))
            loop(2, lambda n: kept(near + n))
        loop(2, near_then_far)

    def forward_layer(layer):
        par = lax.rem(layer, 2)

        def alpha(i):
            @pl.when(layer > 0)
            def _():
                exchange(par, i).wait()
                release(i)
            cos_b, sin_b = rot[layer, 0], rot[layer, 1]
            for local_rows, rows, cols, _c in groups(i):
                re, im = [None] * 8, [None] * 8
                for j in range(4):
                    v = rotate(load_state(par, rows, cols, j), cos_b, sin_b)
                    for half in range(2):
                        n = half * 4 + j
                        pr, pi = v[2 * half], v[2 * half + 1]
                        saved[layer, 0, n, rows, cols] = pr
                        saved[layer, 1, n, rows, cols] = pi
                        c, s = tab[layer, 0, n, rows, cols], tab[layer, 1, n, rows, cols]
                        re[n], im[n] = pr * c + pi * s, pi * c - pr * s
                spread(re, im, local_rows, cols)
            to_state(par, i)
        loop(NUM_CHUNKS, alpha)

        @pl.when((layer >= 2))
        def _():
            stash_out(layer - 2).wait()
        middle(layer, par, True)

        @pl.when(layer < 3)
        def _():
            stash_out(layer).start()

        def gamma_sweep(i):
            from_state(par, i)
            for local_rows, rows, cols, _c in groups(i):
                re, im = gather_big(local_rows, cols)
                for j in range(4):
                    store_state(par, rows, cols, j, (re[j], im[j], re[4 + j], im[4 + j]))

            send(1 - par, i, layer == 0)
        loop(NUM_CHUNKS, gamma_sweep)

    def final(i):
        exchange(1, i).wait()
        release(i)
        energy = jnp.zeros((8, 128), F32)
        grad = jnp.zeros((8, 128), F32)
        cos_b, sin_b = rot[LAYERS, 0], rot[LAYERS, 1]
        for local_rows, rows, cols, crows in groups(i):
            for j in range(4):
                kr, ki, orr, oi = rotate(load_state(1, rows, cols, j), cos_b, sin_b)
                ck, co = cc[0, j, crows, :], cc[2, j, crows, :]
                lam = (ck * kr, ck * ki, co * orr, co * oi)
                energy = energy + fold(lam[0] * kr + lam[1] * ki + lam[2] * orr + lam[3] * oi)
                grad = grad + fold((ck - co) * (kr * oi - ki * orr))
                store_state(1, rows, cols, j, rotate(lam, cos_b, -sin_b))
        acc[0] = acc[0] + energy
        acc[2 * LAYERS] = acc[2 * LAYERS] + grad

        send(0, i)

    def backward_layer(step):
        layer = LAYERS - 1 - step
        par = lax.rem(layer, 2)

        def alpha(i):
            exchange(par, i).wait()

            @pl.when(layer > 0)
            def _():
                release(i)
            for local_rows, rows, cols, _c in groups(i):
                v = [load_state(par, rows, cols, j) for j in range(4)]
                re = [v[j][0] for j in range(4)] + [v[j][2] for j in range(4)]
                im = [v[j][1] for j in range(4)] + [v[j][3] for j in range(4)]
                spread(re, im, local_rows, cols)
            to_state(par, i)
        loop(NUM_CHUNKS, alpha)

        @pl.when(layer < 3)
        def _():
            stash_in(layer).wait()
        total = middle(layer, par, False)
        acc[LAYERS + 1 + layer] = acc[LAYERS + 1 + layer] + total

        @pl.when(layer >= 2)
        def _():
            stash_in(layer - 2).start()

        def gamma_sweep(i):
            from_state(par, i)
            g_sum = jnp.zeros((8, 128), F32)
            b_sum = jnp.zeros((8, 128), F32)
            cos_b, sin_b = rot[layer, 0], rot[layer, 1]
            for local_rows, rows, cols, crows in groups(i):
                re, im = gather_big(local_rows, cols)
                for j in range(4):
                    lam, psi = [], []
                    for half in range(2):
                        n = half * 4 + j
                        c, s = tab[layer, 0, n, rows, cols], tab[layer, 1, n, rows, cols]
                        lr, li = re[n] * c - im[n] * s, im[n] * c + re[n] * s
                        pr, pi = saved[layer, 0, n, rows, cols], saved[layer, 1, n, rows, cols]
                        cost_n = cc[0, j, crows, :] if half == 0 else cc[1 + par, j, crows, :]
                        g_sum = g_sum + fold(cost_n * (lr * pi - li * pr))
                        lam += [lr, li]
                        psi += [pr, pi]
                    b_sum = b_sum + fold(lam[0] * psi[3] - lam[1] * psi[2] + lam[2] * psi[1] - lam[3] * psi[0])
                    store_state(par, rows, cols, j, rotate(lam, cos_b, -sin_b))
            acc[1 + layer] = acc[1 + layer] + 2.0 * g_sum

            @pl.when(layer > 0)
            def _():
                acc[LAYERS + layer] = acc[LAYERS + layer] + b_sum

            @pl.when(layer > 0)
            def _():
                send(1 - par, i)
        loop(NUM_CHUNKS, gamma_sweep)

    def result_copy(a, b):
        return pltpu.make_async_remote_copy(
            src_ref=mine.at[0:NUM_ACC], dst_ref=res.at[qx], send_sem=r_send.at[a * 4 + b], recv_sem=r_recv.at[qx],
            device_id=(inst, a, b), device_id_type=MESH)

    def others(fn):
        for a in range(4):
            for b in range(4):
                @pl.when((qy != a) | (qx != b))
                def _():
                    fn(result_copy(a, b))

    @pl.when(active)
    def _():
        tables()
        arrive()
        loop(LAYERS, forward_layer)
        loop(NUM_CHUNKS, final)
        loop(LAYERS, backward_layer)
        mine[0:NUM_ACC] = jnp.sum(acc[...], axis=1)
        res[qx] = mine[0:NUM_ACC]
        others(lambda copy: copy.start())

    for slot in range(4):
        @pl.when(jnp.logical_not(active & (qx == slot)))
        def _():
            pltpu.make_async_remote_copy(
                src_ref=mine.at[0:NUM_ACC], dst_ref=res.at[slot], send_sem=r_send.at[0], recv_sem=r_recv.at[slot],
                device_id=partner, device_id_type=MESH).wait_recv()

    for s in range(2):
        total = jnp.sum(res[2 * s] + res[2 * s + 1], axis=1, keepdims=True)
        out[s] = jnp.broadcast_to(total, (NUM_ACC, 128))

    for s in range(2):
        @pl.when(jnp.logical_not(is_self(s)))
        def _():
            home_copy(s, cost, qy, qx, c_send.at[s]).wait_send()

        for condition, blocks in relays(s):
            @pl.when(condition)
            def _():
                for r, origin_y, origin_x in blocks:
                    home_copy(s, cc.at[2, r], origin_y, origin_x, relay_send.at[r]).wait_send()

    @pl.when(active)
    def _():
        others(lambda copy: copy.wait_send())


def hadamard():
    index = np.arange(256)
    both = index[:, None] & index[None, :]
    parity = sum((both >> b) & 1 for b in range(8)) & 1
    return jnp.asarray(1.0 - 2.0 * parity, BF16)


def solution(mesh):
    def device_fn(cost, gamma, beta):
        vmem = pltpu.VMEM
        dma = pltpu.SemaphoreType.DMA
        tile = (256, 256)
        out, _ = pl.pallas_call(
            kernel,
            out_shape=(jax.ShapeDtypeStruct((2, NUM_ACC, 128), F32), jax.ShapeDtypeStruct((3, 2, 8) + tile, F32)),
            in_specs=[pl.BlockSpec(memory_space=pl.ANY), pl.BlockSpec(memory_space=pltpu.SMEM),
                      pl.BlockSpec(memory_space=pltpu.SMEM), pl.BlockSpec(memory_space=pltpu.VMEM)],
            out_specs=(pl.BlockSpec(memory_space=pltpu.VMEM), pl.BlockSpec(memory_space=pl.ANY)),
            scratch_shapes=[
                vmem((2, 4) + tile, F32),
                vmem((2, 2, 4) + tile, F32),
                vmem((3, 4, 512, 128), F32),
                vmem((LAYERS, 2, 8) + tile, F32),
                vmem((LAYERS, 2, 8) + tile, F32),
                vmem((2, 2, 8) + tile, F32),
                vmem((LAYERS, 3, 12, 8, 128), F32),
                vmem((LAYERS + 1, 2, 16, 128), F32),
                vmem((NUM_ACC, 8, 128), F32),
                vmem((4,) + tile, F32),
                vmem((4,) + tile, F32),
                vmem((16, CHUNK, 256), F32),
                vmem((2 * NUM_ACC, 128), F32),
                vmem((4, NUM_ACC, 128), F32),
                dma((2,)), dma((2, 4)), dma((4,)), dma((4,)), dma((2, NUM_CHUNKS)), dma((2, NUM_CHUNKS)),
                dma((2,)), dma((2,)), dma((16,)), dma((4,)), dma((2,)), dma((2, len(PARTS))), pltpu.SemaphoreType.REGULAR((NUM_CHUNKS,)),
            ],
            compiler_params=pltpu.CompilerParams(collective_id=0, has_side_effects=True, vmem_limit_bytes=67043328),
        )(cost.reshape(512, 128), gamma, beta, hadamard())
        return out[:, 0, 0], out[:, 1:1 + 2 * LAYERS, 0]

    cost_spec = P(('inst', 'qy', 'qx'))
    angle_spec = P('inst', None)
    return jax.shard_map(device_fn, mesh=mesh, in_specs=(cost_spec, angle_spec, angle_spec), out_specs=(P('inst'), angle_spec), check_vma=False)
```
